8 devices in a mesh: w: 4 (over z, y, x), h: 2 (over core).
Axes of the slice: x: 2, y: 2, z: 1, core: 2. Of those that a mesh axis runs over, the one named last changes fastest.
Arguments:
- x: bfloat16 [1, 64, 1024, 256], P(None, 'h', 'w')
- w1: bfloat16 [3, 3, 256, 256], replicated
- gamma: float32 [256], replicated
- beta: float32 [256], replicated
- w2: bfloat16 [3, 3, 256, 256], replicated
- g: bfloat16 [1, 64, 1024, 256], P(None, 'h', 'w')
Outputs:
- output 1: bfloat16 [1, 64, 1024, 256], P(None, 'h', 'w')
- output 2: bfloat16 [1, 64, 1024, 256], P(None, 'h', 'w')
- output 3: float32 [3, 3, 256, 256], replicated
- output 4: float32 [3, 3, 256, 256], replicated
- output 5: float32 [256], replicated
- output 6: float32 [256], replicated
All inputs are finite; a program needn't handle non-finite values.
Results may differ from the reference program's by a relative error of at most 0.00124822.
Values are sent between devices in bfloat16 or wider.
A program may use at most 1 GiB of HBM per device.

```python
import jax
import jax.numpy as jnp
from jax import lax

B = 1
C = 256
GROUPS = 32
TH = 32
TW = 256
HT = 2
WT = 4
HS = HT * TH
WS = WT * TW
DN = ('NHWC', 'HWIO', 'NHWC')


def setup_inputs(seed: int = 0) -> dict:
    ks = jax.random.split(jax.random.PRNGKey(seed), 6)
    rows = jnp.arange(HS)
    cols = jnp.arange(WS)
    xs = (0.5 + 1.5 * rows / HS)[None, :, None, None]
    x = (jax.random.normal(ks[0], (B, HS, WS, C), jnp.float32) * xs).astype(jnp.bfloat16)
    std = (9 * C) ** -0.5
    w1 = (jax.random.normal(ks[1], (3, 3, C, C), jnp.float32) * std).astype(jnp.bfloat16)
    gamma = 1.0 + 0.3 * jax.random.normal(ks[2], (C,), jnp.float32)
    beta = 0.3 * jax.random.normal(ks[3], (C,), jnp.float32)
    w2 = (jax.random.normal(ks[4], (3, 3, C, C), jnp.float32) * std).astype(jnp.bfloat16)
    edge = ((rows % TH == 0) | (rows % TH == TH - 1))[:, None] | ((cols % TW == 0) | (cols % TW == TW - 1))[None, :]
    gs = jnp.where(edge, 3.0, 1.0)[None, :, :, None]
    g = (jax.random.normal(ks[5], (B, HS, WS, C), jnp.float32) * gs).astype(jnp.bfloat16)
    return {'x': x, 'w1': w1, 'gamma': gamma, 'beta': beta, 'w2': w2, 'g': g}


def _conv(u, w):
    return lax.conv_general_dilated(u.astype(jnp.float32), w.astype(jnp.float32), (1, 1), 'SAME', dimension_numbers=DN)


def _conv_t(v, w):
    return _conv(v, jnp.flip(w, (0, 1)).transpose(0, 1, 3, 2))


def _wgrad(u, v):
    up = jnp.pad(u.astype(jnp.float32), ((0, 0), (1, 1), (1, 1), (0, 0)))
    v32 = v.astype(jnp.float32)
    h, w = v.shape[1], v.shape[2]
    return jnp.stack([jnp.stack([jnp.einsum('bhwc,bhwo->co', up[:, a:a + h, b:b + w], v32) for b in range(3)]) for a in range(3)])


def _norm_act(a, gamma, beta):
    nb, h, w, c = a.shape
    ag = a.reshape(nb, h, w, GROUPS, c // GROUPS)
    mean = ag.mean(axis=(1, 2, 4), keepdims=True)
    var = ((ag - mean) ** 2).mean(axis=(1, 2, 4), keepdims=True)
    n = ((ag - mean) * lax.rsqrt(var + 1e-5)).reshape(a.shape) * gamma + beta
    return jax.nn.gelu(n, approximate=True)


def reference(x, w1, gamma, beta, w2, g):
    a = _conv(x, w1).astype(jnp.bfloat16).astype(jnp.float32)
    zf, vjp = jax.vjp(_norm_act, a, gamma, beta)
    z = zf.astype(jnp.bfloat16)
    y = (_conv(z, w2) + x.astype(jnp.float32)).astype(jnp.bfloat16)
    dz = _conv_t(g, w2)
    dw2 = _wgrad(z, g)
    da, dgamma, dbeta = vjp(dz)
    da = da.astype(jnp.bfloat16)
    dx = (_conv_t(da, w1) + g.astype(jnp.float32)).astype(jnp.bfloat16)
    dw1 = _wgrad(x, da)
    return y, dx, dw1, dw2, dgamma, dbeta
```

```python
import functools

import jax
import jax.numpy as jnp
from jax import lax
from jax.experimental import pallas as pl
from jax.experimental.pallas import tpu as pltpu
from jax.sharding import PartitionSpec as P

GROUPS = 32
EPS = 1e-5
MESH = pl.DeviceIdType.MESH
F32 = jnp.float32
BF16 = jnp.bfloat16
GC0 = 0.7978845608028654
GC1 = 0.044715
TH, TW, C = 32, 256, 256
CG = C // GROUPS
NW, NH = 4, 2
ND = NW * NH
CNT = float(TH * NH * TW * NW * CG)
TB = 16
EXT = TW + 2 * TB
R = 4
NX = 4


def _group_sum(v):
    lane = lax.broadcasted_iota(jnp.int32, v.shape, 1)
    for k in (1, 2, 4):
        up = pltpu.roll(v, C - k, 1)
        down = pltpu.roll(v, k, 1)
        v = v + jnp.where((lane & k) == 0, up, down)
    return v


def _fold8(v):
    return v.reshape(v.shape[0] // 8, 8, C).sum(0)


def kernel(x_hbm, w1_hbm, gam_ref, bet_ref, w2_hbm, g_hbm,
           y_hbm, dx_hbm, dw1_hbm, dw2_hbm, dgam_ref, dbet_ref,
           xn, gn, ux, ug, uz, ud, abuf, dz, vt, w1, w2, w1t, w2t, dw, rd, r1, r2,
           cs, cr, cc, stat, pm, qm,
           in_sem, out_sem, hs_send, hs_recv, st_send, st_recv, ar_send, ar_recv):
    w = lax.axis_index("w")
    h = lax.axis_index("h")
    me = w * NH + h

    rows = TH // NX
    loads = {}
    for q, (src, dst) in enumerate(((x_hbm, xn), (g_hbm, gn))):
        for k in range(NX):
            cp = pltpu.make_async_copy(src.at[pl.ds(k * rows, rows)], dst.at[pl.ds(k * rows, rows)], in_sem.at[q * NX + k])
            cp.start()
            loads[q, k] = cp
        wsrc, wdst = ((w1_hbm, w1), (w2_hbm, w2))[q]
        cp = pltpu.make_async_copy(wsrc, wdst, in_sem.at[2 * NX + q])
        cp.start()
        loads[q, "w"] = cp

    barrier = pltpu.get_barrier_semaphore()
    for k in range(1, ND):
        t = lax.rem(me + k, ND)
        pl.semaphore_signal(barrier, inc=1, device_id={"w": t // NH, "h": lax.rem(t, NH)}, device_id_type=MESH)

    pi = lax.broadcasted_iota(jnp.int32, (EXT, TW), 0)
    pj = lax.broadcasted_iota(jnp.int32, (EXT, TW), 1)
    pm[...] = jnp.where(pj == (pi & 15) * TB + (pi >> 4) - 1, 1.0, 0.0).astype(BF16)
    qi = lax.broadcasted_iota(jnp.int32, (TW, TW), 0)
    qj = lax.broadcasted_iota(jnp.int32, (TW, TW), 1)
    qm[...] = jnp.where(qi == (qj & 15) * TB + (qj >> 4), 1.0, 0.0).astype(BF16)
    for u in (ux, ug, uz, ud):
        u[pl.ds(33 * h, 1)] = jnp.zeros((1, EXT, C), BF16)

    @pl.when(w == 0)
    def _():
        for q in range(4):
            cr[q, 0] = jnp.zeros((TH, C), F32)
            cc[q, 0] = jnp.zeros((8, C), F32)

    @pl.when(w == NW - 1)
    def _():
        for q in range(4):
            cr[q, 1] = jnp.zeros((TH, C), F32)
            cc[q, 1] = jnp.zeros((8, C), F32)

    def to_dev(dw_, dh):
        return {"w": w + dw_, "h": h if dh == 0 else 1 - h}

    def rcopy(src, dst, ss, rs, dev):
        return pltpu.make_async_remote_copy(src_ref=src, dst_ref=dst, send_sem=ss, recv_sem=rs, device_id=dev, device_id_type=MESH)

    def halo_copies(q, u):
        row = rcopy(u.at[pl.ds(32 - 31 * h, 1)], u.at[pl.ds(33 * h, 1)], hs_send.at[q, 0], hs_recv.at[q, 0], to_dev(0, 1))
        slab = pl.ds(pl.multiple_of(24 * (1 - h), 8), 8)
        left = [rcopy(cs.at[q, 0], cr.at[q, 1], hs_send.at[q, 1], hs_recv.at[q, 1], to_dev(-1, 0)),
                rcopy(cs.at[q, 0, slab], cc.at[q, 1], hs_send.at[q, 2], hs_recv.at[q, 2], to_dev(-1, 1))]
        right = [rcopy(cs.at[q, 1], cr.at[q, 0], hs_send.at[q, 3], hs_recv.at[q, 3], to_dev(1, 0)),
                 rcopy(cs.at[q, 1, slab], cc.at[q, 0], hs_send.at[q, 4], hs_recv.at[q, 4], to_dev(1, 1))]
        return row, left, right

    def halo_start(q, u):
        row, left, right = halo_copies(q, u)
        row.start()

        @pl.when(w > 0)
        def _():
            for cp in left:
                cp.start()

        @pl.when(w < NW - 1)
        def _():
            for cp in right:
                cp.start()

    sub = lax.broadcasted_iota(jnp.int32, (TB, C), 0)

    def put(u, r, lo, hi):
        b0 = u[r, 0:TB, :].astype(F32)
        u[r, 0:TB, :] = jnp.where(sub == 0, lo, b0).astype(BF16)
        b1 = u[r, TW + TB:EXT, :].astype(F32)
        u[r, TW + TB:EXT, :] = jnp.where(sub == TB - 1, hi, b1).astype(BF16)

    def halo_finish(q, u):
        row, left, right = halo_copies(q, u)
        row.wait()

        @pl.when(w > 0)
        def _():
            for cp in left:
                cp.wait_send()
            for cp in right:
                cp.wait_recv()

        @pl.when(w < NW - 1)
        def _():
            for cp in right:
                cp.wait_send()
            for cp in left:
                cp.wait_recv()

        def step(k, _):
            for i in range(4):
                r = k * 4 + i
                put(u, r + 1, cr[q, 0, pl.ds(r, 1), :], cr[q, 1, pl.ds(r, 1), :])
            return 0
        lax.fori_loop(0, TH // 4, step, 0)
        put(u, 33 * (1 - h), cc[q, 0, pl.ds(7 * h, 1), :], cc[q, 1, pl.ds(7 * h, 1), :])

    def permute_in(q, src, u):
        for k in range(NX):
            loads[q, k].wait()

            def step(i, _):
                for d in range(4):
                    r = k * rows + i * 4 + d
                    v = jnp.dot(pm[...], src[r], preferred_element_type=F32)
                    u[r + 1] = v.astype(BF16)
                    cs[q, 0, pl.ds(r, 1), :] = v[TB:TB + 1]
                    cs[q, 1, pl.ds(r, 1), :] = v[TW + TB - 1:TW + TB]
                return 0
            lax.fori_loop(0, rows // 4, step, 0)

    def pad_blocks(q, u, r, first, last):
        u[r + 1, 0:TB, :] = jnp.where(sub == 0, 0.0, pltpu.roll(last, 1, 0)).astype(BF16)
        u[r + 1, TW + TB:EXT, :] = jnp.where(sub == TB - 1, 0.0, pltpu.roll(first, TB - 1, 0)).astype(BF16)
        cs[q, 0, pl.ds(r, 1), :] = first[0:1]
        cs[q, 1, pl.ds(r, 1), :] = last[TB - 1:TB]

    def conv(u, wt, r0):
        lhs = jnp.concatenate([u[pl.ds(r0 + a, R), TB * b:TB * b + TW, :].reshape(R * TW, C) for a in range(3) for b in range(3)], axis=1)
        return jnp.dot(lhs, wt[...], preferred_element_type=F32)

    def stat_copies(q):
        out = []
        for k in range(1, ND):
            t = lax.rem(me + k, ND)
            out.append(rcopy(stat.at[q, me], stat.at[q, me], st_send.at[q, k], st_recv.at[q, me], {"w": t // NH, "h": lax.rem(t, NH)}))
        return out

    def stat_start(q, a, b):
        stat[q, me] = jnp.concatenate([a, b, jnp.zeros((6, C), F32)], axis=0)
        for cp in stat_copies(q):
            cp.start()

    def stat_finish(q):
        for k in range(1, ND):
            t = lax.rem(me + k, ND)
            rcopy(stat.at[q, t], stat.at[q, t], st_send.at[q, k], st_recv.at[q, t], {"w": t // NH, "h": lax.rem(t, NH)}).wait_recv()
        for cp in stat_copies(q):
            cp.wait_send()
        tot = stat[q, 0]
        for k in range(1, ND):
            tot = tot + stat[q, k]
        return tot

    xb = lax.rem(w, 2)
    yb = w // 2
    dev_x = {"w": w + 1 - 2 * xb, "h": h}
    dev_y = {"w": w + 2 - 4 * yb, "h": h}
    dev_c = {"w": w, "h": 1 - h}

    def part(n, off, size):
        return dw.at[n, :, pl.ds(pl.multiple_of(off, 16), size), :]

    def half(n, off, size):
        return rd.at[n, :, pl.ds(pl.multiple_of(off, 16), size), :]

    def ar_copies(n):
        mine, other = 128 * h, 128 * (1 - h)
        c = []
        s = [0]

        def add(src, dst, dev):
            k = s[0]
            c.append(lambda: rcopy(src, dst, ar_send.at[n, k], ar_recv.at[n, k], dev))
            s[0] += 1
        add(part(n, other, 128), rd.at[n], dev_c)
        add(part(n, mine + 32 * (1 - xb), 32), r1.at[n, 0], dev_x)
        add(part(n, mine + 64 + 32 * (1 - yb), 32), r1.at[n, 1], dev_y)
        add(part(n, mine + 32 * xb + 16 * (1 - yb), 16), r2.at[n, 0], dev_y)
        add(part(n, mine + 64 + 32 * yb + 16 * (1 - xb), 16), r2.at[n, 1], dev_x)
        o0, o1 = 32 * xb + 16 * yb, 64 + 32 * yb + 16 * xb
        add(half(n, o0, 16), half(n, o0, 16), dev_y)
        add(half(n, o1, 16), half(n, o1, 16), dev_x)
        add(half(n, 32 * xb, 32), half(n, 32 * xb, 32), dev_x)
        add(half(n, 64 + 32 * yb, 32), half(n, 64 + 32 * yb, 32), dev_y)
        out = (dw2_hbm, dw1_hbm)[n].at[:, pl.ds(pl.multiple_of(mine, 128), 128), :]
        add(rd.at[n], out, dev_c)
        c.append(lambda: pltpu.make_async_copy(rd.at[n], out, in_sem.at[n]))
        return c

    AR_SETS = ((0,), (1, 2), (3, 4), (5, 6), (7, 8), (9, 10))

    def accumulate(n, off, size, src, into=None):
        def step(t, _):
            sl = pl.ds(pl.multiple_of(128 * h + off, 16), size)
            v = dw[n, t, sl, :] + src[t]
            if into is None:
                dw[n, t, sl, :] = v
            else:
                rd[n, t, pl.ds(pl.multiple_of(off, 16), size), :] = v
            return 0
        lax.fori_loop(0, 9, step, 0)

    def ar_step(n, k):
        cps = ar_copies(n)
        if k > 0:
            for i in AR_SETS[k - 1]:
                cps[i]().wait()
        if k == 1:
            accumulate(n, 0, 128, rd.at[n])
        if k == 2:
            accumulate(n, 32 * xb, 32, r1.at[n, 0])
            accumulate(n, 64 + 32 * yb, 32, r1.at[n, 1])
        if k == 3:
            accumulate(n, 32 * xb + 16 * yb, 16, r2.at[n, 0], rd)
            accumulate(n, 64 + 32 * yb + 16 * xb, 16, r2.at[n, 1], rd)
        if k < 6:
            for i in AR_SETS[k]:
                cps[i]().start()

    def wgrad(n, u):
        def step(t, _):
            a = t // 3
            b = lax.rem(t, 3)
            rhs = u[pl.ds(a, TH), pl.ds(pl.multiple_of(TB * b, TB), TW), :].reshape(TH * TW, C)
            acc = jnp.dot(vt[...], rhs, preferred_element_type=F32)
            dw[n, t] = acc.T
            return 0
        lax.fori_loop(0, 9, step, 0)

    pl.semaphore_wait(barrier, ND - 1)
    permute_in(0, xn, ux)
    halo_start(0, ux)
    permute_in(1, gn, ug)
    halo_start(1, ug)
    loads[0, "w"].wait()
    loads[1, "w"].wait()

    def wtrans(t, _):
        w1t[pl.ds(pl.multiple_of((8 - t) * C, C), C), :] = w1[pl.ds(pl.multiple_of(t * C, C), C), :].T
        w2t[pl.ds(pl.multiple_of((8 - t) * C, C), C), :] = w2[pl.ds(pl.multiple_of(t * C, C), C), :].T
        return 0
    lax.fori_loop(0, 9, wtrans, 0)
    halo_finish(0, ux)

    def conv1_step(k, carry):
        s1, s2 = carry
        a = conv(ux, w1, k * R).astype(BF16)
        abuf[pl.ds(k * R, R)] = a.reshape(R, TW, C)
        af = a.astype(F32)
        return s1 + _fold8(af), s2 + _fold8(af * af)
    zero = jnp.zeros((8, C), F32)
    s1, s2 = lax.fori_loop(0, TH // R, conv1_step, (zero, zero))
    stat_start(0, s1.sum(0, keepdims=True), s2.sum(0, keepdims=True))
    halo_finish(1, ug)

    def convt2_step(k, _):
        dz[pl.ds(k * R, R)] = conv(ug, w2t, k * R).reshape(R, TW, C)
        for i in range(R):
            r = k * R + i
            vt[:, pl.ds(pl.multiple_of(r * TW, TW), TW)] = ug[r + 1, TB:TB + TW, :].T
        return 0
    lax.fori_loop(0, TH // R, convt2_step, 0)

    tot = _group_sum(stat_finish(0)) / CNT
    mean = tot[0:1]
    rstd = lax.rsqrt(tot[1:2] - mean * mean + EPS)
    gam = gam_ref[...]
    bet = bet_ref[...]

    SB = 32

    def act_step(r, carry):
        t0, t1 = carry
        first = last = None
        for i in range(TW // SB):
            p = i * SB
            xhat = (abuf[r, p:p + SB, :].astype(F32) - mean) * rstd
            n = xhat * gam + bet
            n2 = n * n
            th = jnp.tanh(GC0 * (n + GC1 * (n * n2)))
            hp = 0.5 + 0.5 * th
            z = n * hp
            dg = hp + (0.5 * GC0) * n * (1.0 - th * th) * (1.0 + (3.0 * GC1) * n2)
            dn = dz[r, p:p + SB, :] * dg
            dz[r, p:p + SB, :] = dn
            uz[r + 1, TB + p:TB + p + SB, :] = z.astype(BF16)
            t0 = t0 + _fold8(dn * xhat)
            t1 = t1 + _fold8(dn)
            if i == 0:
                first = z[0:TB]
            if i == TW // SB - 1:
                last = z[SB - TB:SB]
        pad_blocks(2, uz, r, first, last)
        return t0, t1
    t0, t1 = lax.fori_loop(0, TH, act_step, (zero, zero))
    stat_start(1, t0.sum(0, keepdims=True), t1.sum(0, keepdims=True))
    halo_start(2, uz)
    halo_finish(2, uz)
    wgrad(0, uz)
    ar_step(0, 0)

    tot = stat_finish(1)
    dgam_ref[...] = tot[0:1]
    dbet_ref[...] = tot[1:2]
    us = _group_sum(tot * gam) / CNT
    k0 = rstd * gam
    k1 = rstd * us[0:1]
    k2 = rstd * us[1:2]

    def da_step(r, _):
        first = last = None
        for i in range(TW // SB):
            p = i * SB
            xhat = (abuf[r, p:p + SB, :].astype(F32) - mean) * rstd
            d = dz[r, p:p + SB, :] * k0 - k2 - xhat * k1
            ud[r + 1, TB + p:TB + p + SB, :] = d.astype(BF16)
            if i == 0:
                first = d[0:TB]
            if i == TW // SB - 1:
                last = d[SB - TB:SB]
        pad_blocks(3, ud, r, first, last)
        vt[:, pl.ds(pl.multiple_of(r * TW, TW), TW)] = ud[r + 1, TB:TB + TW, :].T
        return 0
    lax.fori_loop(0, TH, da_step, 0)
    halo_start(3, ud)
    ar_step(0, 1)
    wgrad(1, ux)
    halo_finish(3, ud)
    ar_step(1, 0)
    ar_step(0, 2)

    def out_copy(q, k):
        src, dst = ((xn, y_hbm), (gn, dx_hbm))[q]
        return pltpu.make_async_copy(src.at[pl.ds(k * R, R)], dst.at[pl.ds(k * R, R)], out_sem.at[q, k])

    def out_step(q, u, wt, res, out, k):
        acc = conv(u, wt, k * R).reshape(R, TW, C)
        for i in range(R):
            r = k * R + i
            v = (acc[i] + res[r + 1, TB:TB + TW, :].astype(F32)).astype(BF16)
            out[r] = jnp.dot(qm[...], v, preferred_element_type=F32).astype(BF16)
        out_copy(q, k).start()

    def y_step(k, _):
        out_step(0, uz, w2, ux, xn, k)
        return 0

    def dx_step(k, _):
        out_step(1, ud, w1t, ug, gn, k)
        return 0
    hk = TH // R // 2
    lax.fori_loop(0, hk, y_step, 0)
    ar_step(0, 3)
    ar_step(1, 1)
    lax.fori_loop(hk, TH // R, y_step, 0)
    ar_step(0, 4)
    ar_step(1, 2)
    lax.fori_loop(0, hk, dx_step, 0)
    ar_step(0, 5)
    ar_step(1, 3)
    lax.fori_loop(hk, TH // R, dx_step, 0)
    ar_step(0, 6)
    ar_step(1, 4)
    ar_step(1, 5)
    ar_step(1, 6)
    for q in range(2):
        for k in range(TH // R):
            out_copy(q, k).wait()


def solution(mesh):
    tile = P(None, 'h', 'w', None)

    def body(x, w1, gamma, beta, w2, g):
        anyspec = pl.BlockSpec(memory_space=pl.ANY)
        vspec = pl.BlockSpec(memory_space=pltpu.VMEM)
        S = jax.ShapeDtypeStruct
        V = pltpu.VMEM
        DMA = pltpu.SemaphoreType.DMA
        img = (TH, TW, C)
        uimg = (TH + 2, EXT, C)
        y, dx, dw1, dw2, dgam, dbet = pl.pallas_call(
            kernel,
            out_shape=(S(img, BF16), S(img, BF16), S((9, C, C), F32), S((9, C, C), F32), S((1, C), F32), S((1, C), F32)),
            in_specs=[anyspec, anyspec, vspec, vspec, anyspec, anyspec],
            out_specs=(anyspec, anyspec, anyspec, anyspec, vspec, vspec),
            scratch_shapes=[
                V(img, BF16), V(img, BF16), V(uimg, BF16), V(uimg, BF16), V(uimg, BF16), V(uimg, BF16),
                V(img, BF16), V(img, F32), V((C, TH * TW), BF16),
                V((9 * C, C), BF16), V((9 * C, C), BF16), V((9 * C, C), BF16), V((9 * C, C), BF16),
                V((2, 9, C, C), F32), V((2, 9, 128, C), F32), V((2, 2, 9, 32, C), F32), V((2, 2, 9, 16, C), F32),
                V((4, 2, TH, C), F32), V((4, 2, TH, C), F32), V((4, 2, 8, C), F32), V((2, ND, 8, C), F32),
                V((EXT, TW), BF16), V((TW, TW), BF16),
                DMA((2 * NX + 2,)), DMA((2, TH // R)), DMA((4, 5)), DMA((4, 5)), DMA((2, ND)), DMA((2, ND)), DMA((2, 10)), DMA((2, 10)),
            ],
            compiler_params=pltpu.CompilerParams(collective_id=0, has_side_effects=True, vmem_limit_bytes=67043328),
        )(x.reshape(img), w1.reshape(9 * C, C), gamma.reshape(1, C), beta.reshape(1, C), w2.reshape(9 * C, C), g.reshape(img))
        return (y.reshape(x.shape), dx.reshape(x.shape), dw1.reshape(w1.shape), dw2.reshape(w2.shape), dgam.reshape(C), dbet.reshape(C))

    return jax.shard_map(body, mesh=mesh, in_specs=(tile, P(), P(), P(), P(), tile), out_specs=(tile, tile, P(), P(), P(), P()), check_vma=False)
```

```python
import functools

import jax
import jax.numpy as jnp
from jax import lax
from jax.experimental import pallas as pl
from jax.experimental.pallas import tpu as pltpu
from jax.sharding import PartitionSpec as P

GROUPS = 32
EPS = 1e-5
MESH = pl.DeviceIdType.MESH
F32 = jnp.float32
BF16 = jnp.bfloat16
GC0 = 0.7978845608028654
GC1 = 0.044715
TH, TW, C = 32, 256, 256
CG = C // GROUPS
NW, NH = 4, 2
ND = NW * NH
CNT = float(TH * NH * TW * NW * CG)
TB = 16
EXT = TW + 2 * TB
R = 4
NX = 2


def _group_sum(v):
    lane = lax.broadcasted_iota(jnp.int32, v.shape, 1)
    for k in (1, 2, 4):
        up = pltpu.roll(v, C - k, 1)
        down = pltpu.roll(v, k, 1)
        v = v + jnp.where((lane & k) == 0, up, down)
    return v


def _fold8(v):
    return v.reshape(v.shape[0] // 8, 8, C).sum(0)


def kernel(x_hbm, w1_hbm, gam_hbm, bet_hbm, w2_hbm, g_hbm,
           y_hbm, dx_hbm, dw1_hbm, dw2_hbm, dgam_hbm, dbet_hbm,
           xn, gn, ux, ug, uz, ud, abuf, ost, dz, raw, w1, w2, w1t, w2t, dw, rd, r1, r2,
           cs, cr, cc, stat, pm, vec,
           in_sem, vec_sem, out_sem, hs_send, hs_recv, st_send, st_recv, ar_send, ar_recv):
    w = lax.axis_index("w")
    h = lax.axis_index("h")
    me = w * NH + h

    rows = TH // NX
    loads = {}
    for q, (src, dst) in enumerate(((x_hbm, xn), (g_hbm, gn))):
        for k in range(NX):
            cp = pltpu.make_async_copy(src.at[pl.ds(k * rows, rows)], dst.at[pl.ds(k * rows, rows)], in_sem.at[q * NX + k])
            cp.start()
            loads[q, k] = cp
        wsrc, wdst = ((w1_hbm, w1), (w2_hbm, w2))[q]
        cp = pltpu.make_async_copy(wsrc, wdst, in_sem.at[2 * NX + q])
        cp.start()
        loads[q, "w"] = cp
        cp = pltpu.make_async_copy((gam_hbm, bet_hbm)[q], vec.at[q], vec_sem.at[q])
        cp.start()
        loads[q, "v"] = cp

    barrier = pltpu.get_barrier_semaphore()
    for k in range(1, ND):
        t = lax.rem(me + k, ND)
        pl.semaphore_signal(barrier, inc=1, device_id={"w": t // NH, "h": lax.rem(t, NH)}, device_id_type=MESH)

    pi = lax.broadcasted_iota(jnp.int32, (EXT, TW), 0)
    pj = lax.broadcasted_iota(jnp.int32, (EXT, TW), 1)
    pm[...] = jnp.where(pj == (pi & 15) * TB + (pi >> 4) - 1, 1.0, 0.0).astype(BF16)
    for u in (ux, ug, uz, ud):
        u[pl.ds(33 * h, 1)] = jnp.zeros((1, EXT, C), BF16)

    @pl.when(w == 0)
    def _():
        for q in range(4):
            cr[q, 0] = jnp.zeros((TH, C), F32)
            cc[q, 0] = jnp.zeros((8, C), F32)

    @pl.when(w == NW - 1)
    def _():
        for q in range(4):
            cr[q, 1] = jnp.zeros((TH, C), F32)
            cc[q, 1] = jnp.zeros((8, C), F32)

    def to_dev(dw_, dh):
        return {"w": w + dw_, "h": h if dh == 0 else 1 - h}

    def rcopy(src, dst, ss, rs, dev):
        return pltpu.make_async_remote_copy(src_ref=src, dst_ref=dst, send_sem=ss, recv_sem=rs, device_id=dev, device_id_type=MESH)

    def halo_copies(q, u):
        slab = pl.ds(pl.multiple_of(24 * (1 - h), 8), 8)

        def make(m, src, dst, dev):
            return lambda: rcopy(src, dst, hs_send.at[q, m], hs_recv.at[q, m], dev)
        row = make(0, u.at[pl.ds(32 - 31 * h, 1)], u.at[pl.ds(33 * h, 1)], to_dev(0, 1))
        left = [make(1, cs.at[q, 0], cr.at[q, 1], to_dev(-1, 0)), make(2, cs.at[q, 0, slab], cc.at[q, 1], to_dev(-1, 1))]
        right = [make(3, cs.at[q, 1], cr.at[q, 0], to_dev(1, 0)), make(4, cs.at[q, 1, slab], cc.at[q, 0], to_dev(1, 1))]
        return row, left, right

    def halo_start(q, u):
        row, left, right = halo_copies(q, u)
        row().start()

        @pl.when(w > 0)
        def _():
            for cp in left:
                cp().start()

        @pl.when(w < NW - 1)
        def _():
            for cp in right:
                cp().start()

    sub = lax.broadcasted_iota(jnp.int32, (TB, C), 0)

    def put(u, r, lo, hi):
        b0 = u[r, 0:TB, :].astype(F32)
        u[r, 0:TB, :] = jnp.where(sub == 0, lo, b0).astype(BF16)
        b1 = u[r, TW + TB:EXT, :].astype(F32)
        u[r, TW + TB:EXT, :] = jnp.where(sub == TB - 1, hi, b1).astype(BF16)

    def halo_row(q, u):
        halo_copies(q, u)[0]().wait()

    def halo_cols(q, u):
        _, left, right = halo_copies(q, u)

        @pl.when(w > 0)
        def _():
            for cp in left:
                cp().wait_send()
            for cp in right:
                cp().wait_recv()

        @pl.when(w < NW - 1)
        def _():
            for cp in right:
                cp().wait_send()
            for cp in left:
                cp().wait_recv()

        def step(k, _):
            for i in range(4):
                r = k * 4 + i
                put(u, r + 1, cr[q, 0, pl.ds(r, 1), :], cr[q, 1, pl.ds(r, 1), :])
            return 0
        lax.fori_loop(0, TH // 4, step, 0)
        put(u, 33 * (1 - h), cc[q, 0, pl.ds(7 * h, 1), :], cc[q, 1, pl.ds(7 * h, 1), :])

    def permute_in(q, src, u):
        for k in range(NX):
            loads[q, k].wait()

            def step(i, _):
                for d in range(16):
                    r = k * rows + i * 16 + d
                    v = jnp.dot(pm[...], src[r], preferred_element_type=F32)
                    u[r + 1] = v.astype(BF16)
                    cs[q, 0, pl.ds(r, 1), :] = v[TB:TB + 1]
                    cs[q, 1, pl.ds(r, 1), :] = v[TW + TB - 1:TW + TB]
                return 0
            lax.fori_loop(0, rows // 16, step, 0)

    def pad_blocks(q, u, r, first, last):
        u[r + 1, 0:TB, :] = jnp.where(sub == 0, 0.0, pltpu.roll(last, 1, 0)).astype(BF16)
        u[r + 1, TW + TB:EXT, :] = jnp.where(sub == TB - 1, 0.0, pltpu.roll(first, TB - 1, 0)).astype(BF16)
        cs[q, 0, pl.ds(r, 1), :] = first[0:1]
        cs[q, 1, pl.ds(r, 1), :] = last[TB - 1:TB]

    def conv(u, wt, r0, R=R):
        lhs = jnp.concatenate([u[pl.ds(r0 + a, R), TB * b:TB * b + TW, :].reshape(R * TW, C) for a in range(3) for b in range(3)], axis=1)
        return jnp.dot(lhs, wt[...], preferred_element_type=F32)

    def stat_copies(q):
        out = []
        for k in range(1, ND):
            t = lax.rem(me + k, ND)
            out.append(rcopy(stat.at[q, me], stat.at[q, me], st_send.at[q, k], st_recv.at[q, me], {"w": t // NH, "h": lax.rem(t, NH)}))
        return out

    def stat_start(q, a, b):
        stat[q, me] = jnp.concatenate([a, b, jnp.zeros((6, C), F32)], axis=0)
        for cp in stat_copies(q):
            cp.start()

    def stat_finish(q):
        for k in range(1, ND):
            t = lax.rem(me + k, ND)
            rcopy(stat.at[q, t], stat.at[q, t], st_send.at[q, k], st_recv.at[q, t], {"w": t // NH, "h": lax.rem(t, NH)}).wait_recv()
        for cp in stat_copies(q):
            cp.wait_send()
        tot = stat[q, 0]
        for k in range(1, ND):
            tot = tot + stat[q, k]
        return tot

    xb = lax.rem(w, 2)
    yb = w // 2
    dev_x = {"w": w + 1 - 2 * xb, "h": h}
    dev_y = {"w": w + 2 - 4 * yb, "h": h}
    dev_c = {"w": w, "h": 1 - h}

    BS = (1, 0, 2)

    def part(n, c, off, size):
        return dw.at[n, c, :, pl.ds(pl.multiple_of(off, 16), size), :]

    def half(n, c, off, size):
        return rd.at[n, c, :, pl.ds(pl.multiple_of(off, 16), size), :]

    def ar_copies(n, c):
        mine, other = 128 * h, 128 * (1 - h)
        o0, o1 = 32 * xb + 16 * yb, 64 + 32 * yb + 16 * xb
        q0, q1 = 32 * xb, 64 + 32 * yb
        out = (dw2_hbm, dw1_hbm)[n].at[:, BS[c], pl.ds(pl.multiple_of(mine, 128), 128), :]
        plan = (
            (part(n, c, other, 128), rd.at[n, c], dev_c),
            (part(n, c, mine + 32 * (1 - xb), 32), r1.at[n, c, 0], dev_x),
            (part(n, c, mine + 64 + 32 * (1 - yb), 32), r1.at[n, c, 1], dev_y),
            (part(n, c, mine + 32 * xb + 16 * (1 - yb), 16), r2.at[n, c, 0], dev_y),
            (part(n, c, mine + 64 + 32 * yb + 16 * (1 - xb), 16), r2.at[n, c, 1], dev_x),
            (half(n, c, o0, 16), half(n, c, o0, 16), dev_y),
            (half(n, c, o1, 16), half(n, c, o1, 16), dev_x),
            (half(n, c, q0, 32), half(n, c, q0, 32), dev_x),
            (half(n, c, q1, 32), half(n, c, q1, 32), dev_y),
            (rd.at[n, c], out, dev_c),
        )

        def make(k):
            src, dst, dev = plan[k]
            return lambda: rcopy(src, dst, ar_send.at[n, c, k], ar_recv.at[n, c, k], dev)
        return [make(k) for k in range(10)] + [lambda: pltpu.make_async_copy(rd.at[n, c], out, in_sem.at[n * 3 + c])]

    AR_SETS = ((0,), (1, 2), (3, 4), (5, 6), (7, 8), (9, 10))

    def accumulate(n, c, off, size, src, into=None):
        sl = pl.ds(pl.multiple_of(128 * h + off, 16), size)
        for t in range(3):
            v = dw[n, c, t, sl, :] + src[t]
            if into is None:
                dw[n, c, t, sl, :] = v
            else:
                rd[n, c, t, pl.ds(pl.multiple_of(off, 16), size), :] = v

    def ar_step(n, c, k):
        with jax.named_scope(f"ar_{n}_{c}_{k}"):
            cps = ar_copies(n, c)
            if k > 0:
                for i in AR_SETS[k - 1]:
                    cps[i]().wait()
            if k == 1:
                accumulate(n, c, 0, 128, rd.at[n, c])
            if k == 2:
                accumulate(n, c, 32 * xb, 32, r1.at[n, c, 0])
                accumulate(n, c, 64 + 32 * yb, 32, r1.at[n, c, 1])
            if k == 3:
                accumulate(n, c, 32 * xb + 16 * yb, 16, r2.at[n, c, 0], rd)
                accumulate(n, c, 64 + 32 * yb + 16 * xb, 16, r2.at[n, c, 1], rd)
            if k < 6:
                for i in AR_SETS[k]:
                    cps[i]().start()

    LAG = (0, 1, 5, 9, 12, 16, 18)
    START = (4, 7, 9, 13, 16, 18)
    SLOTS = {(i // 3, i % 3): [min(s_ + l_, 34) for l_ in LAG] for i, s_ in enumerate(START)}
    plan_at = {}
    for (n_, c_), at_ in SLOTS.items():
        for k_, s_ in enumerate(at_):
            plan_at.setdefault(s_, []).append((n_, c_, k_))

    def sums_at(base, lo, hi, i):
        for sl in range(lo, hi):
            if sl + base in plan_at:
                def _(todo=plan_at[sl + base]):
                    for n, c, k in sorted(todo, key=lambda e: -e[2]):
                        ar_step(n, c, k)
                pl.when(i == sl)(_)

    def perm3(i):
        return (3 * i * i - 5 * i + 2) // 2

    def turn(n, t):
        dw[n, t // 3, perm3(lax.rem(t, 3))] = raw[...].T

    def tap(n, u, vt, t):
        turn(n, lax.max(t - 1, 0))
        a = perm3(lax.rem(t, 3))
        b = perm3(t // 3)
        rhs = u[pl.ds(a, TH), pl.ds(pl.multiple_of(TB * b, TB), TW), :].reshape(TH * TW, C)
        lhs = jnp.concatenate([vt[r] for r in range(TH)], axis=1)
        raw[...] = jnp.dot(lhs, rhs, preferred_element_type=F32)

    with jax.named_scope("barrier"):
        pl.semaphore_wait(barrier, ND - 1)
    with jax.named_scope("perm_x"):
        permute_in(0, xn, ux)
    with jax.named_scope("hstart"):
        halo_start(0, ux)
    with jax.named_scope("perm_g"):
        permute_in(1, gn, ug)
    with jax.named_scope("hstart"):
        halo_start(1, ug)
    loads[0, "w"].wait()
    loads[1, "w"].wait()

    def wtrans(t, _):
        w1t[pl.ds(pl.multiple_of((8 - t) * C, C), C), :] = w1[pl.ds(pl.multiple_of(t * C, C), C), :].T
        w2t[pl.ds(pl.multiple_of((8 - t) * C, C), C), :] = w2[pl.ds(pl.multiple_of(t * C, C), C), :].T
        return 0
    with jax.named_scope("wtrans"):
        lax.fori_loop(0, 9, wtrans, 0)
    with jax.named_scope("hfin_x"):
        halo_row(0, ux)
        halo_cols(0, ux)

    def conv1_step(k, carry):
        s1, s2 = carry
        a = conv(ux, w1, k * 8, 8).astype(BF16)
        abuf[pl.ds(k * 8, 8)] = a.reshape(8, TW, C)
        af = a.astype(F32)
        return s1 + _fold8(af), s2 + _fold8(af * af)
    zero = jnp.zeros((8, C), F32)
    with jax.named_scope("conv1"):
        s1, s2 = lax.fori_loop(0, TH // 8, conv1_step, (zero, zero))
    with jax.named_scope("ststart"):
        stat_start(0, s1.sum(0, keepdims=True), s2.sum(0, keepdims=True))
    with jax.named_scope("hfin_g"):
        halo_row(1, ug)
        halo_cols(1, ug)

    def convt2(k):
        dz[pl.ds(k * R, R)] = conv(ug, w2t, k * R).reshape(R, TW, C)
        for i in range(R):
            r = k * R + i
            gn[r] = ug[r + 1, TB:TB + TW, :].T

    def convt2_first(k, _):
        convt2(k)
        return 0
    with jax.named_scope("convt2"):
        lax.fori_loop(0, 4, convt2_first, 0)

    with jax.named_scope("stat0"):
        tot = _group_sum(stat_finish(0)) / CNT
    mean = tot[0:1]
    rstd = lax.rsqrt(tot[1:2] - mean * mean + EPS)
    loads[0, "v"].wait()
    loads[1, "v"].wait()
    gam = vec[0]
    bet = vec[1]
    ngain = rstd * gam

    SB = 32

    def gate(r, p):
        am = abuf[r, p:p + SB, :].astype(F32) - mean
        n = am * ngain + bet
        n2 = n * n
        th = jnp.tanh(n * (n2 * (GC0 * GC1) + GC0))
        return am, n, n2, 0.5 * th + 0.5

    def z_row(r):
        first = last = None
        for i in range(TW // SB):
            p = i * SB
            am, n, n2, hp = gate(r, p)
            z = n * hp
            uz[r + 1, TB + p:TB + p + SB, :] = z.astype(BF16)
            if i == 0:
                first = z[0:TB]
            if i == TW // SB - 1:
                last = z[SB - TB:SB]
        pad_blocks(2, uz, r, first, last)

    def convt2_z(k, _):
        with jax.named_scope("convt2z"):
            for i in range(8):
                z_row((k - 4) * 8 + i)
            convt2(k)
        return 0
    lax.fori_loop(4, 8, convt2_z, 0)
    with jax.named_scope("hstart"):
        halo_start(2, uz)

    def dn_row(r, carry):
        t0, t1 = carry
        for i in range(TW // SB):
            p = i * SB
            am, n, n2, hp = gate(r, p)
            dg = hp + n * ((hp - hp * hp) * (n2 * (6.0 * GC0 * GC1) + 2.0 * GC0))
            dn = dz[r, p:p + SB, :] * dg
            dz[r, p:p + SB, :] = dn
            t0 = t0 + _fold8(dn * am)
            t1 = t1 + _fold8(dn)
        return t0, t1

    raw[...] = jnp.zeros((C, C), F32)

    def wgrad2_dn(t, carry):
        @pl.when(t == 1)
        def _():
            with jax.named_scope("hrow_z"):
                halo_row(2, uz)

        @pl.when(t == 3)
        def _():
            with jax.named_scope("hcol_z"):
                halo_cols(2, uz)
        with jax.named_scope("tap2dn"):
            for i in range(8):
                carry = dn_row(t * 8 + i, carry)
            tap(0, uz, gn, t)
        return carry
    t0, t1 = lax.fori_loop(0, 4, wgrad2_dn, (zero, zero))
    with jax.named_scope("ststart"):
        stat_start(1, t0.sum(0, keepdims=True) * rstd, t1.sum(0, keepdims=True))

    def wgrad2_plain(t, _):
        sums_at(0, 4, 7, t)
        with jax.named_scope("tap2"):
            tap(0, uz, gn, t)
        return 0
    lax.fori_loop(4, 7, wgrad2_plain, 0)

    with jax.named_scope("stat1"):
        tot = stat_finish(1)
    vec[2] = tot[0:1]
    vec[3] = tot[1:2]
    outv = [pltpu.make_async_copy(vec.at[2 + q], (dgam_hbm, dbet_hbm)[q], vec_sem.at[q]) for q in range(2)]
    for cp in outv:
        cp.start()
    us = _group_sum(tot * gam) / CNT
    k0 = rstd * gam
    k1 = rstd * rstd * us[0:1]
    k2 = rstd * us[1:2]

    def da_row(r):
        first = last = None
        for i in range(TW // SB):
            p = i * SB
            am = abuf[r, p:p + SB, :].astype(F32) - mean
            d = dz[r, p:p + SB, :] * k0 - (am * k1 + k2)
            ud[r + 1, TB + p:TB + p + SB, :] = d.astype(BF16)
            if i == 0:
                first = d[0:TB]
            if i == TW // SB - 1:
                last = d[SB - TB:SB]
        pad_blocks(3, ud, r, first, last)
        xn[r] = ud[r + 1, TB:TB + TW, :].T

    def wgrad2_da(t, _):
        sums_at(0, 7, 9, t)
        with jax.named_scope("tap2da"):
            for i in range(16):
                da_row((t - 7) * 16 + i)
            tap(0, uz, gn, t)
        return 0
    lax.fori_loop(7, 9, wgrad2_da, 0)
    with jax.named_scope("hstart"):
        halo_start(3, ud)
    turn(0, 8)

    def wgrad1_step(t, _):
        sums_at(9, 0, 9, t)
        with jax.named_scope("tap1"):
            tap(1, ux, xn, t)
        return 0
    lax.fori_loop(0, 9, wgrad1_step, 0)
    turn(1, 8)
    with jax.named_scope("hfin_d"):
        halo_row(3, ud)
        halo_cols(3, ud)

    def out_copy(q, k):
        src, dst = ((abuf, y_hbm), (ost, dx_hbm))[q]
        return pltpu.make_async_copy(src.at[pl.ds(k * R, R)], dst.at[pl.ds(k * R, R)], out_sem.at[q, k])

    def out_step(q, u, wt, res, out, k):
        acc = conv(u, wt, k * R).reshape(R, TW, C)
        v = acc + res[pl.ds(k * R + 1, R), TB:TB + TW, :].astype(F32)
        out[pl.ds(k * R, R)] = v.astype(BF16)
        out_copy(q, k).start()

    def y_step(k, _):
        sums_at(26, 0, 8, k)
        with jax.named_scope("y"):
            out_step(0, uz, w2, ux, abuf, k)
        return 0

    def dx_step(k, _):
        sums_at(18, 0, 8, k)
        with jax.named_scope("dx"):
            out_step(1, ud, w1t, ug, ost, k)
        return 0
    lax.fori_loop(0, TH // R, dx_step, 0)
    lax.fori_loop(0, TH // R, y_step, 0)
    for sl in range(34, 40):
        for n, c, k in plan_at.get(sl, ()):
            ar_step(n, c, k)
    with jax.named_scope("outw"):
        for q in range(2):
            outv[q].wait()
            for k in range(TH // R):
                out_copy(q, k).wait()


def finish(y_ref, dx_ref, w1_ref, w2_ref, ga_ref, be_ref, yo, dxo, w1o, w2o, gao, beo, qm):
    qi = lax.broadcasted_iota(jnp.int32, (TW, TW), 0)
    qj = lax.broadcasted_iota(jnp.int32, (TW, TW), 1)

    @pl.when(pl.program_id(0) == 0)
    def _():
        qm[...] = jnp.where(qi == (qj & 15) * TB + (qj >> 4), 1.0, 0.0).astype(BF16)
    for src, dst in ((y_ref, yo), (dx_ref, dxo)):
        for r in range(src.shape[0]):
            dst[r] = jnp.dot(qm[...], src[r], preferred_element_type=F32).astype(BF16)
    w1o[...] = w1_ref[...]
    w2o[...] = w2_ref[...]
    gao[...] = ga_ref[...]
    beo[...] = be_ref[...]


def solution(mesh):
    tile = P(None, 'h', 'w', None)

    def body(x, w1, gamma, beta, w2, g):
        anyspec = pl.BlockSpec(memory_space=pl.ANY)
        S = jax.ShapeDtypeStruct
        V = pltpu.VMEM
        DMA = pltpu.SemaphoreType.DMA
        img = (TH, TW, C)
        uimg = (TH + 2, EXT, C)
        out = pl.pallas_call(
            kernel,
            out_shape=(S(img, BF16), S(img, BF16), S((3, 3, C, C), F32), S((3, 3, C, C), F32), S((1, C), F32), S((1, C), F32)),
            in_specs=[anyspec] * 6,
            out_specs=(anyspec,) * 6,
            scratch_shapes=[
                V(img, BF16), V(img, BF16), V(uimg, BF16), V(uimg, BF16), V(uimg, BF16), V(uimg, BF16),
                V(img, BF16), V(img, BF16), V(img, F32), V((C, C), F32),
                V((9 * C, C), BF16), V((9 * C, C), BF16), V((9 * C, C), BF16), V((9 * C, C), BF16),
                V((2, 3, 3, C, C), F32), V((2, 3, 3, 128, C), F32), V((2, 3, 2, 3, 32, C), F32), V((2, 3, 2, 3, 16, C), F32),
                V((4, 2, TH, C), F32), V((4, 2, TH, C), F32), V((4, 2, 8, C), F32), V((2, ND, 8, C), F32),
                V((EXT, TW), BF16), V((4, 1, C), F32),
                DMA((2 * NX + 2,)), DMA((2,)), DMA((2, TH // R)), DMA((4, 5)), DMA((4, 5)), DMA((2, ND)), DMA((2, ND)), DMA((2, 3, 10)), DMA((2, 3, 10)),
            ],
            compiler_params=pltpu.CompilerParams(collective_id=0, has_side_effects=True, vmem_limit_bytes=67043328),
        )(x.reshape(img), w1.reshape(9 * C, C), gamma.reshape(1, C), beta.reshape(1, C), w2.reshape(9 * C, C), g.reshape(img))
        y, dx, dw1, dw2, dgam, dbet = out
        steps = 8
        wrows = (9 * C, C)
        ispec = pl.BlockSpec((TH // steps, TW, C), lambda i: (i, 0, 0))
        wspec = pl.BlockSpec((9 * C // steps, C), lambda i: (i, 0))
        cspec = pl.BlockSpec((1, C), lambda i: (0, 0))
        y, dx, dw1, dw2, dgam, dbet = pl.pallas_call(
            finish,
            grid=(steps,),
            out_shape=(S(img, BF16), S(img, BF16), S(wrows, F32), S(wrows, F32), S((1, C), F32), S((1, C), F32)),
            in_specs=[ispec, ispec, wspec, wspec, cspec, cspec],
            out_specs=(ispec, ispec, wspec, wspec, cspec, cspec),
            scratch_shapes=[V((TW, TW), BF16)],
        )(y, dx, dw1.reshape(wrows), dw2.reshape(wrows), dgam, dbet)
        return (y.reshape(x.shape), dx.reshape(x.shape), dw1.reshape(w1.shape), dw2.reshape(w2.shape), dgam.reshape(C), dbet.reshape(C))

    return jax.shard_map(body, mesh=mesh, in_specs=(tile, P(), P(), P(), P(), tile), out_specs=(tile, tile, P(), P(), P(), P()), check_vma=False)
```

```python
import functools

import jax
import jax.numpy as jnp
from jax import lax
from jax.experimental import pallas as pl
from jax.experimental.pallas import tpu as pltpu
from jax.sharding import PartitionSpec as P

GROUPS = 32
EPS = 1e-5
MESH = pl.DeviceIdType.MESH
F32 = jnp.float32
BF16 = jnp.bfloat16
GC0 = 0.7978845608028654
GC1 = 0.044715
TH, TW, C = 32, 256, 256
CG = C // GROUPS
NW, NH = 4, 2
ND = NW * NH
CNT = float(TH * NH * TW * NW * CG)
TB = 16
EXT = TW + 2 * TB
R = 4
NX = 2


def _group_sum(v):
    lane = lax.broadcasted_iota(jnp.int32, v.shape, 1)
    for k in (1, 2, 4):
        up = pltpu.roll(v, C - k, 1)
        down = pltpu.roll(v, k, 1)
        v = v + jnp.where((lane & k) == 0, up, down)
    return v


def _loop(lo, hi, f):
    def body(i, c):
        f(i)
        return c
    lax.fori_loop(lo, hi, body, 0)


def _row(v):
    return v.sum(0, keepdims=True)


def _fold8(v):
    return v.reshape(v.shape[0] // 8, 8, C).sum(0)


def kernel(x_hbm, w1_hbm, gam_hbm, bet_hbm, w2_hbm, g_hbm,
           y_hbm, dx_hbm, dw1_hbm, dw2_hbm, dgam_hbm, dbet_hbm,
           xn, gn, ux, ug, uz, ud, abuf, ost, dz, raw, w1, w2, w1t, w2t, dw, rd, r1, r2,
           cs, cr, cc, stat, pm, vec,
           in_sem, vec_sem, out_sem, hs_send, hs_recv, st_send, st_recv, ar_send, ar_recv):
    w = lax.axis_index("w")
    h = lax.axis_index("h")
    me = w * NH + h

    rows = TH // NX
    loads = {}
    for q, (src, dst) in enumerate(((x_hbm, xn), (g_hbm, gn))):
        for k in range(NX):
            cp = pltpu.make_async_copy(src.at[pl.ds(k * rows, rows)], dst.at[pl.ds(k * rows, rows)], in_sem.at[q * NX + k])
            cp.start()
            loads[q, k] = cp
        wsrc, wdst = ((w1_hbm, w1), (w2_hbm, w2))[q]
        cp = pltpu.make_async_copy(wsrc, wdst, in_sem.at[2 * NX + q])
        cp.start()
        loads[q, "w"] = cp
        cp = pltpu.make_async_copy((gam_hbm, bet_hbm)[q], vec.at[q], vec_sem.at[q])
        cp.start()
        loads[q, "v"] = cp

    barrier = pltpu.get_barrier_semaphore()
    for k in range(1, ND):
        t = lax.rem(me + k, ND)
        pl.semaphore_signal(barrier, inc=1, device_id={"w": t // NH, "h": lax.rem(t, NH)}, device_id_type=MESH)

    pi = lax.broadcasted_iota(jnp.int32, (EXT, TW), 0)
    pj = lax.broadcasted_iota(jnp.int32, (EXT, TW), 1)
    pm[:, :] = jnp.where(pj == (pi & 15) * TB + (pi >> 4) - 1, 1.0, 0.0).astype(BF16)
    for u in (ux, ug, uz, ud):
        u[pl.ds(33 * h, 1)] = jnp.zeros((1, EXT, C), BF16)

    def no_neighbour(side):
        cr[:, side] = jnp.zeros((4, TH, C), F32)
        cc[:, side] = jnp.zeros((4, 8, C), F32)
    pl.when(w == 0)(lambda: no_neighbour(0))
    pl.when(w == NW - 1)(lambda: no_neighbour(1))

    def to_dev(dw_, dh):
        return {"w": w + dw_, "h": h if dh == 0 else 1 - h}

    def rcopy(src, dst, ss, rs, dev):
        return pltpu.make_async_remote_copy(src_ref=src, dst_ref=dst, send_sem=ss, recv_sem=rs, device_id=dev, device_id_type=MESH)

    def halo_copies(q, u):
        slab = pl.ds(pl.multiple_of(24 * (1 - h), 8), 8)

        def make(m, src, dst, dev):
            return lambda: rcopy(src, dst, hs_send.at[q, m], hs_recv.at[q, m], dev)
        row = make(0, u.at[pl.ds(32 - 31 * h, 1)], u.at[pl.ds(33 * h, 1)], to_dev(0, 1))
        left = [make(1, cs.at[q, 0], cr.at[q, 1], to_dev(-1, 0)), make(2, cs.at[q, 0, slab], cc.at[q, 1], to_dev(-1, 1))]
        right = [make(3, cs.at[q, 1], cr.at[q, 0], to_dev(1, 0)), make(4, cs.at[q, 1, slab], cc.at[q, 0], to_dev(1, 1))]
        return row, left, right

    def halo_start(q, u, row_too=True):
        row, left, right = halo_copies(q, u)
        if row_too:
            row().start()

        @pl.when(w > 0)
        def _():
            for cp in left:
                cp().start()

        @pl.when(w < NW - 1)
        def _():
            for cp in right:
                cp().start()

    sub = lax.broadcasted_iota(jnp.int32, (TB, C), 0)

    def put(u, r, lo, hi):
        b0 = u[r, :TB, :].astype(F32)
        u[r, :TB, :] = jnp.where(sub == 0, lo, b0).astype(BF16)
        b1 = u[r, TW + TB:, :].astype(F32)
        u[r, TW + TB:, :] = jnp.where(sub == TB - 1, hi, b1).astype(BF16)

    def halo_row(q, u):
        halo_copies(q, u)[0]().wait()

    def halo_cols(q, u):
        _, left, right = halo_copies(q, u)

        @pl.when(w > 0)
        def _():
            for cp in left:
                cp().wait_send()
            for cp in right:
                cp().wait_recv()

        @pl.when(w < NW - 1)
        def _():
            for cp in right:
                cp().wait_send()
            for cp in left:
                cp().wait_recv()

        def step(k):
            for i in range(4):
                r = k * 4 + i
                put(u, r + 1, cr[q, 0, pl.ds(r, 1), :], cr[q, 1, pl.ds(r, 1), :])
        _loop(0, TH // 4, step)
        put(u, 33 * (1 - h), cc[q, 0, pl.ds(7 * h, 1), :], cc[q, 1, pl.ds(7 * h, 1), :])

    def permute_in(q, src, u):
        for k in range(NX):
            if q == 1:
                loads[q, k].wait()

            def step(i):
                for d in range(16):
                    r = k * rows + i * 16 + d
                    v = jnp.dot(pm[:, :], src[r], preferred_element_type=F32)
                    u[r + 1] = v.astype(BF16)
                    if q == 1:
                        cs[q, 0, pl.ds(r, 1), :] = v[TB:TB + 1]
                        cs[q, 1, pl.ds(r, 1), :] = v[TW + TB - 1:TW + TB]
            _loop(0, rows // 16, step)

    def pad_blocks(q, u, r, first, last):
        u[r + 1, :TB, :] = jnp.where(sub == 0, 0.0, pltpu.roll(last, 1, 0)).astype(BF16)
        u[r + 1, TW + TB:, :] = jnp.where(sub == TB - 1, 0.0, pltpu.roll(first, TB - 1, 0)).astype(BF16)
        cs[q, 0, pl.ds(r, 1), :] = first[0:1]
        cs[q, 1, pl.ds(r, 1), :] = last[TB - 1:TB]

    def conv(u, wt, r0, R=R):
        lhs = jnp.concatenate([u[pl.ds(r0 + a, R), TB * b:TB * b + TW, :].reshape(R * TW, C) for a in range(3) for b in range(3)], axis=1)
        return jnp.dot(lhs, wt[:, :], preferred_element_type=F32)

    def stat_copies(q):
        out = []
        for k in range(1, ND):
            t = lax.rem(me + k, ND)
            out.append(rcopy(stat.at[q, me], stat.at[q, me], st_send.at[q], st_recv.at[q], {"w": t // NH, "h": lax.rem(t, NH)}))
        return out

    def stat_start(q, a, b):
        stat[q, me] = jnp.concatenate([a, b, jnp.zeros((6, C), F32)], axis=0)
        for cp in stat_copies(q):
            cp.start()

    def stat_finish(q):
        others = stat.at[q, pl.ds(0, ND - 1)]
        rcopy(others, others, st_send.at[q], st_recv.at[q], dev_c).wait()
        tot = stat[q, 0]
        for k in range(1, ND):
            tot = tot + stat[q, k]
        return tot

    xb = lax.rem(w, 2)
    yb = w // 2
    dev_x = {"w": w + 1 - 2 * xb, "h": h}
    dev_y = {"w": w + 2 - 4 * yb, "h": h}
    dev_c = {"w": w, "h": 1 - h}

    BS = (1, 0, 2)

    def part(n, c, off, size):
        return dw.at[n, c, :, pl.ds(pl.multiple_of(off, 16), size), :]

    def half(n, c, off, size):
        return rd.at[n, c, :, pl.ds(pl.multiple_of(off, 16), size), :]

    def ar_copies(n, c):
        mine, other = 128 * h, 128 * (1 - h)
        o0, o1 = 32 * xb + 16 * yb, 64 + 32 * yb + 16 * xb
        q0, q1 = 32 * xb, 64 + 32 * yb
        out = (dw2_hbm, dw1_hbm)[n].at[:, BS[c], pl.ds(pl.multiple_of(mine, 128), 128), :]
        plan = (
            (part(n, c, other, 128), rd.at[n, c], dev_c),
            (part(n, c, mine + 32 * (1 - xb), 32), r1.at[n, c, 0], dev_x),
            (part(n, c, mine + 64 + 32 * (1 - yb), 32), r1.at[n, c, 1], dev_y),
            (part(n, c, mine + 32 * xb + 16 * (1 - yb), 16), r2.at[n, c, 0], dev_y),
            (part(n, c, mine + 64 + 32 * yb + 16 * (1 - xb), 16), r2.at[n, c, 1], dev_x),
            (half(n, c, o0, 16), half(n, c, o0, 16), dev_y),
            (half(n, c, o1, 16), half(n, c, o1, 16), dev_x),
            (half(n, c, q0, 32), half(n, c, q0, 32), dev_x),
            (half(n, c, q1, 32), half(n, c, q1, 32), dev_y),
            (rd.at[n, c], out, dev_c),
        )

        def make(k):
            src, dst, dev = plan[k]
            return lambda: rcopy(src, dst, ar_send.at[n, c, k % 2], ar_recv.at[n, c, k], dev)
        return [make(k) for k in range(10)] + [lambda: pltpu.make_async_copy(rd.at[n, c], out, in_sem.at[n * 3 + c])]

    AR_SETS = ((0,), (1, 2), (3, 4), (5, 6), (7, 8), (9, 10))

    def accumulate(n, c, off, size, src, into=None):
        sl = pl.ds(pl.multiple_of(128 * h + off, 16), size)
        for t in range(3):
            v = dw[n, c, t, sl, :] + src[t]
            if into is None:
                dw[n, c, t, sl, :] = v
            else:
                rd[n, c, t, pl.ds(pl.multiple_of(off, 16), size), :] = v

    def ar_step(n, c, k):
        with jax.named_scope(f"ar_{n}_{c}_{k}"):
            cps = ar_copies(n, c)
            if k > 0:
                for i in AR_SETS[k - 1]:
                    cps[i]().wait()
            if k == 1:
                accumulate(n, c, 0, 128, rd.at[n, c])
            if k == 2:
                accumulate(n, c, 32 * xb, 32, r1.at[n, c, 0])
                accumulate(n, c, 64 + 32 * yb, 32, r1.at[n, c, 1])
            if k == 3:
                accumulate(n, c, 32 * xb + 16 * yb, 16, r2.at[n, c, 0], rd)
                accumulate(n, c, 64 + 32 * yb + 16 * xb, 16, r2.at[n, c, 1], rd)
            if k < 6:
                for i in AR_SETS[k]:
                    cps[i]().start()

    SLOTS = "347:?FI79<?CKQ:;>AHNQ@BGJMQRCEILNQREFILORR"
    plan_at = {}
    for i_, ch_ in enumerate(SLOTS):
        plan_at.setdefault(ord(ch_) - ord("0"), []).append((i_ // 21, i_ // 7 % 3, i_ % 7))

    def sums_at(base, lo, hi, i):
        for sl in range(lo, hi):
            if sl + base in plan_at:
                def _(todo=plan_at[sl + base]):
                    for n, c, k in sorted(todo, key=lambda e: -e[2]):
                        ar_step(n, c, k)
                pl.when(i == sl)(_)

    def perm3(i):
        return (3 * i * i - 5 * i + 2) // 2

    def turn(n, t):
        dw[n, t // 3, perm3(t % 3)] = raw[:, :].T

    def tap(n, u, vt, t, first):
        turn(n, lax.max(t - 1, first))
        rhs = u[pl.ds(perm3(t % 3), TH), pl.ds(pl.multiple_of(TB * perm3(t // 3), TB), TW), :].reshape(TH * TW, C)
        lhs = jnp.concatenate([vt[r] for r in range(TH)], axis=1)
        raw[:, :] = jnp.dot(lhs, rhs, preferred_element_type=F32)

    def x_edges(i):
        for d in range(8):
            r = i * 8 + d
            cs[0, 0, pl.ds(r, 1), :] = xn[r, :TB, :].astype(F32)[:1]
            cs[0, 1, pl.ds(r, 1), :] = xn[r, TW - TB:, :].astype(F32)[TB - 1:]
    with jax.named_scope("edges"):
        for k in range(NX):
            loads[0, k].wait()
        _loop(0, TH // 8, x_edges)
    with jax.named_scope("barrier"):
        pl.semaphore_wait(barrier, ND - 1)
    halo_start(0, ux, False)
    with jax.named_scope("perm_x"):
        permute_in(0, xn, ux)
    halo_copies(0, ux)[0]().start()
    with jax.named_scope("perm_g"):
        permute_in(1, gn, ug)
    halo_start(1, ug)
    loads[0, "w"].wait()
    loads[1, "w"].wait()
    with jax.named_scope("hfin_x"):
        halo_row(0, ux)
        halo_cols(0, ux)

    def wtrans(k):
        for i in range(3):
            t = lax.min(k * 3 + i, 8)
            src, dst = pl.ds(pl.multiple_of(t * C, C), C), pl.ds(pl.multiple_of((8 - t) * C, C), C)
            w1t[dst, :] = w1[src, :].T
            w2t[dst, :] = w2[src, :].T

    def conv1_step(k, carry):
        s1, s2 = carry
        wtrans(k)
        a = conv(ux, w1, k * 8, 8).astype(BF16)
        abuf[pl.ds(k * 8, 8)] = a.reshape(8, TW, C)
        af = a.astype(F32)
        return s1 + _fold8(af), s2 + _fold8(af * af)
    zero = jnp.zeros((8, C), F32)
    with jax.named_scope("conv1"):
        s1, s2 = lax.fori_loop(0, TH // 8, conv1_step, (zero, zero))
    with jax.named_scope("ststart"):
        stat_start(0, _row(s1), _row(s2))
    with jax.named_scope("hfin_g"):
        halo_row(1, ug)
        halo_cols(1, ug)

    def convt2(k):
        dz[pl.ds(k * R, R)] = conv(ug, w2t, k * R).reshape(R, TW, C)
        for i in range(R):
            r = k * R + i
            gn[r] = ug[r + 1, TB:TB + TW, :].T

    def convt2_first(k):
        convt2(k)
    with jax.named_scope("convt2"):
        _loop(0, 4, convt2_first)

    with jax.named_scope("stat0"):
        tot = _group_sum(stat_finish(0)) / CNT
    mean = tot[0:1]
    rstd = lax.rsqrt(tot[1:2] - mean * mean + EPS)
    loads[0, "v"].wait()
    loads[1, "v"].wait()
    gam = vec[0]
    bet = vec[1]
    ngain = rstd * gam

    SB = 32

    def gate(r, sl):
        am = abuf[r, sl, :].astype(F32) - mean
        n = am * ngain + bet
        n2 = n * n
        th = jnp.tanh(n * (n2 * (GC0 * GC1) + GC0))
        return am, n, n2, 0.5 * th + 0.5

    def slope(n, n2, hp):
        return hp + n * ((hp - hp * hp) * (n2 * (6.0 * GC0 * GC1) + 2.0 * GC0))

    def act_row(r, carry, do_z, do_dn):
        t0, t1 = carry
        first = last = None
        for i in range(TW // SB):
            sl = pl.ds(i * SB, SB)
            am, n, n2, hp = gate(r, sl)
            if do_z:
                z = n * hp
                uz[r + 1, pl.ds(TB + i * SB, SB), :] = z.astype(BF16)
                first = z[:TB] if first is None else first
                last = z[SB - TB:]
            if do_dn:
                dn = dz[r, sl, :] * slope(n, n2, hp)
                dz[r, sl, :] = dn
                t0 = t0 + _fold8(dn * am)
                t1 = t1 + _fold8(dn)
        if do_z:
            pad_blocks(2, uz, r, first, last)
        return t0, t1

    def convt2_z(k):
        with jax.named_scope("convt2z"):
            for i in range(8):
                act_row((k - 4) * 8 + i, (zero, zero), True, False)
            convt2(k)
    _loop(4, 8, convt2_z)
    with jax.named_scope("hstart"):
        halo_start(2, uz)
    raw[:, :] = jnp.zeros((C, C), F32)

    def tap2(lo, hi, first, rows, carry):
        def step(t, c):
            sums_at(0, lo, hi, t)
            if lo == 0:
                @pl.when(t == 1)
                def _():
                    with jax.named_scope("hrow_z"):
                        halo_row(2, uz)
            with jax.named_scope("tap2"):
                for i in range(rows):
                    c = act_row((t - lo) * rows + i, c, False, True)
                tap(0, uz, gn, t, first)
            return c
        return lax.fori_loop(lo, hi, step, carry)

    sums = tap2(0, 3, 0, 0, (zero, zero))
    turn(0, 2)
    with jax.named_scope("hcol_z"):
        halo_cols(2, uz)
    sums = tap2(3, 7, 3, 8, sums)
    with jax.named_scope("ststart"):
        stat_start(1, _row(sums[0]) * rstd, _row(sums[1]))
    tap2(7, 9, 3, 0, zero)
    turn(0, 8)

    def out_copy(q, k):
        src, dst = (ost if q == 0 else abuf, (y_hbm, dx_hbm)[q])
        return pltpu.make_async_copy(src.at[pl.ds(k * R, R)], dst.at[pl.ds(k * R, R)], out_sem.at[q])

    def out_step(q, u, wt, res, out, k):
        acc = conv(u, wt, k * R).reshape(R, TW, C)
        v = acc + res[pl.ds(k * R + 1, R), TB:TB + TW, :].astype(F32)
        out[pl.ds(k * R, R)] = v.astype(BF16)
        out_copy(q, k).start()

    def y_rows(lo, hi, slot, extra=None):
        def step(k):
            sums_at(slot - lo, lo, hi, k)
            with jax.named_scope("y"):
                if extra is not None:
                    extra(k)
                out_step(0, uz, w2, ux, ost, k)
        _loop(lo, hi, step)
    y_rows(0, 1, 9)

    with jax.named_scope("stat1"):
        tot = stat_finish(1)
    vec[2] = tot[0:1]
    vec[3] = tot[1:2]
    outv = [pltpu.make_async_copy(vec.at[2 + q], (dgam_hbm, dbet_hbm)[q], vec_sem.at[q]) for q in range(2)]
    for cp in outv:
        cp.start()
    us = _group_sum(tot * gam) / CNT
    k0 = rstd * gam
    k1 = rstd * rstd * us[0:1]
    k2 = rstd * us[1:2]

    def da_row(r):
        first = last = None
        for i in range(TW // SB):
            sl = pl.ds(i * SB, SB)
            am = abuf[r, sl, :].astype(F32) - mean
            d = dz[r, sl, :] * k0 - (am * k1 + k2)
            ud[r + 1, pl.ds(TB + i * SB, SB), :] = d.astype(BF16)
            first = d[:TB] if first is None else first
            last = d[SB - TB:]
        pad_blocks(3, ud, r, first, last)
        xn[r] = ud[r + 1, TB:TB + TW, :].T

    def da_rows(k):
        for i in range(16):
            da_row((k - 1) * 16 + i)
    y_rows(1, 3, 10, da_rows)
    with jax.named_scope("hstart"):
        halo_start(3, ud)

    def wgrad1_step(t):
        sums_at(12, 0, 9, t)
        with jax.named_scope("tap1"):
            tap(1, ux, xn, t, 0)
    _loop(0, 9, wgrad1_step)
    turn(1, 8)
    with jax.named_scope("hfin_d"):
        halo_row(3, ud)
        halo_cols(3, ud)

    def dx_step(k):
        sums_at(21, 0, 8, k)
        with jax.named_scope("dx"):
            out_step(1, ud, w1t, ug, abuf, k)

    _loop(0, TH // R, dx_step)
    y_rows(3, 8, 29)
    for n, c, k in sorted(plan_at[34], key=lambda e: e[2]):
        ar_step(n, c, k)
    with jax.named_scope("outw"):
        for q in range(2):
            outv[q].wait()
            src, dst = (ost if q == 0 else abuf, (y_hbm, dx_hbm)[q])
            pltpu.make_async_copy(src, dst, out_sem.at[q]).wait()


def finish(y_ref, dx_ref, w1_ref, w2_ref, ga_ref, be_ref, yo, dxo, w1o, w2o, gao, beo, qm):
    qi = lax.broadcasted_iota(jnp.int32, (TW, TW), 0)
    qj = lax.broadcasted_iota(jnp.int32, (TW, TW), 1)

    @pl.when(pl.program_id(0) == 0)
    def _():
        qm[:, :] = jnp.where(qi == (qj & 15) * TB + (qj >> 4), 1.0, 0.0).astype(BF16)
    for src, dst in ((y_ref, yo), (dx_ref, dxo)):
        for r in range(src.shape[0]):
            dst[r] = jnp.dot(qm[:, :], src[r], preferred_element_type=F32).astype(BF16)
    w1o[:, :] = w1_ref[:, :]
    w2o[:, :] = w2_ref[:, :]
    gao[:, :] = ga_ref[:, :]
    beo[:, :] = be_ref[:, :]


def solution(mesh):
    tile = P(None, 'h', 'w', None)

    def body(x, w1, gamma, beta, w2, g):
        anyspec = pl.BlockSpec(memory_space=pl.ANY)
        S = jax.ShapeDtypeStruct
        V = pltpu.VMEM
        DMA = pltpu.SemaphoreType.DMA
        img = (TH, TW, C)
        uimg = (TH + 2, EXT, C)
        out = pl.pallas_call(
            kernel,
            out_shape=(S(img, BF16), S(img, BF16), S((3, 3, C, C), F32), S((3, 3, C, C), F32), S((1, C), F32), S((1, C), F32)),
            in_specs=[anyspec] * 6,
            out_specs=(anyspec,) * 6,
            scratch_shapes=[
                V(img, BF16), V(img, BF16), V(uimg, BF16), V(uimg, BF16), V(uimg, BF16), V(uimg, BF16),
                V(img, BF16), V(img, BF16), V(img, F32), V((C, C), F32),
                V((9 * C, C), BF16), V((9 * C, C), BF16), V((9 * C, C), BF16), V((9 * C, C), BF16),
                V((2, 3, 3, C, C), F32), V((2, 3, 3, 128, C), F32), V((2, 3, 2, 3, 32, C), F32), V((2, 3, 2, 3, 16, C), F32),
                V((4, 2, TH, C), F32), V((4, 2, TH, C), F32), V((4, 2, 8, C), F32), V((2, ND, 8, C), F32),
                V((EXT, TW), BF16), V((4, 1, C), F32),
                DMA((2 * NX + 2,)), DMA((2,)), DMA((2,)), DMA((4, 5)), DMA((4, 5)), DMA((2,)), DMA((2,)), DMA((2, 3, 2)), DMA((2, 3, 10)),
            ],
            compiler_params=pltpu.CompilerParams(collective_id=0, has_side_effects=True, vmem_limit_bytes=67043328),
        )(x.reshape(img), w1.reshape(9 * C, C), gamma.reshape(1, C), beta.reshape(1, C), w2.reshape(9 * C, C), g.reshape(img))
        y, dx, dw1, dw2, dgam, dbet = out
        steps = 2
        wrows = (9 * C, C)
        ispec = pl.BlockSpec((TH // steps, TW, C), lambda i: (i, 0, 0))
        wspec = pl.BlockSpec((9 * C // steps, C), lambda i: (i, 0))
        cspec = pl.BlockSpec((1, C), lambda i: (0, 0))
        y, dx, dw1, dw2, dgam, dbet = pl.pallas_call(
            finish,
            grid=(steps,),
            out_shape=(S(img, BF16), S(img, BF16), S(wrows, F32), S(wrows, F32), S((1, C), F32), S((1, C), F32)),
            in_specs=[ispec, ispec, wspec, wspec, cspec, cspec],
            out_specs=(ispec, ispec, wspec, wspec, cspec, cspec),
            scratch_shapes=[V((TW, TW), BF16)],
        )(y, dx, dw1.reshape(wrows), dw2.reshape(wrows), dgam, dbet)
        return (y.reshape(x.shape), dx.reshape(x.shape), dw1.reshape(w1.shape), dw2.reshape(w2.shape), dgam.reshape(C), dbet.reshape(C))

    return jax.shard_map(body, mesh=mesh, in_specs=(tile, P(), P(), P(), P(), tile), out_specs=(tile, tile, P(), P(), P(), P()), check_vma=False)
```

```python
import functools

import jax
import jax.numpy as jnp
from jax import lax
from jax.experimental import pallas as pl
from jax.experimental.pallas import tpu as pltpu
from jax.sharding import PartitionSpec as P

GROUPS = 32
EPS = 1e-5
MESH = pl.DeviceIdType.MESH
F32 = jnp.float32
BF16 = jnp.bfloat16
GC0 = 0.7978845608028654
GC1 = 0.044715
TH, TW, C = 32, 256, 256
CG = C // GROUPS
NW, NH = 4, 2
ND = NW * NH
CNT = float(TH * NH * TW * NW * CG)
TB = 16
EXT = TW + 2 * TB
R = 4
NX = 2


def _group_sum(v):
    lane = lax.broadcasted_iota(jnp.int32, v.shape, 1)
    for k in (1, 2, 4):
        up = pltpu.roll(v, C - k, 1)
        down = pltpu.roll(v, k, 1)
        v = v + jnp.where((lane & k) == 0, up, down)
    return v


def _loop(lo, hi, f):
    def body(i, c):
        f(i)
        return c
    lax.fori_loop(lo, hi, body, 0)


def _row(v):
    return v.sum(0, keepdims=True)


def _fold8(v):
    return v.reshape(v.shape[0] // 8, 8, C).sum(0)


def kernel(x_hbm, w1_hbm, gam_hbm, bet_hbm, w2_hbm, g_hbm,
           y_hbm, dx_hbm, dw1_hbm, dw2_hbm, dgam_hbm, dbet_hbm,
           xn, gn, ux, ug, uz, ud, abuf, ost, dz, raw, w1, w2, w1t, w2t, dw, rd, r1, r2,
           cs, cr, cc, stat, pm, vec,
           in_sem, vec_sem, out_sem, hs_send, hs_recv, st_send, st_recv, ar_send, ar_recv):
    w = lax.axis_index("w")
    h = lax.axis_index("h")
    me = w * NH + h

    rows = TH // NX
    loads = {}
    for q, (src, dst) in enumerate(((x_hbm, xn), (g_hbm, gn))):
        for k in range(NX):
            cp = pltpu.make_async_copy(src.at[pl.ds(k * rows, rows)], dst.at[pl.ds(k * rows, rows)], in_sem.at[q * NX + k])
            cp.start()
            loads[q, k] = cp
        wsrc, wdst = ((w1_hbm, w1), (w2_hbm, w2))[q]
        cp = pltpu.make_async_copy(wsrc, wdst, in_sem.at[2 * NX + q])
        cp.start()
        loads[q, "w"] = cp
        cp = pltpu.make_async_copy((gam_hbm, bet_hbm)[q], vec.at[q], vec_sem.at[q])
        cp.start()
        loads[q, "v"] = cp

    barrier = pltpu.get_barrier_semaphore()
    for k in range(1, ND):
        t = lax.rem(me + k, ND)
        pl.semaphore_signal(barrier, inc=1, device_id={"w": t // NH, "h": lax.rem(t, NH)}, device_id_type=MESH)

    pi = lax.broadcasted_iota(jnp.int32, (EXT, TW), 0)
    pj = lax.broadcasted_iota(jnp.int32, (EXT, TW), 1)
    pm[:, :] = jnp.where(pj == (pi & 15) * TB + (pi >> 4) - 1, 1.0, 0.0).astype(BF16)
    for u in (ux, ug, uz, ud):
        u[pl.ds(33 * h, 1)] = jnp.zeros((1, EXT, C), BF16)

    def no_neighbour(side):
        cr[:, side] = jnp.zeros((4, TH, C), F32)
        cc[:, side] = jnp.zeros((4, 8, C), F32)
    pl.when(w == 0)(lambda: no_neighbour(0))
    pl.when(w == NW - 1)(lambda: no_neighbour(1))

    def to_dev(dw_, dh):
        return {"w": w + dw_, "h": h if dh == 0 else 1 - h}

    def rcopy(src, dst, ss, rs, dev):
        return pltpu.make_async_remote_copy(src_ref=src, dst_ref=dst, send_sem=ss, recv_sem=rs, device_id=dev, device_id_type=MESH)

    def halo_copies(q, u):
        slab = pl.ds(pl.multiple_of(24 * (1 - h), 8), 8)

        def make(m, src, dst, dev):
            return lambda: rcopy(src, dst, hs_send.at[q, m], hs_recv.at[q, m], dev)
        row = make(0, u.at[pl.ds(32 - 31 * h, 1)], u.at[pl.ds(33 * h, 1)], to_dev(0, 1))
        left = [make(1, cs.at[q, 0], cr.at[q, 1], to_dev(-1, 0)), make(2, cs.at[q, 0, slab], cc.at[q, 1], to_dev(-1, 1))]
        right = [make(3, cs.at[q, 1], cr.at[q, 0], to_dev(1, 0)), make(4, cs.at[q, 1, slab], cc.at[q, 0], to_dev(1, 1))]
        return row, left, right

    def halo_start(q, u, row_too=True):
        row, left, right = halo_copies(q, u)
        if row_too:
            row().start()

        @pl.when(w > 0)
        def _():
            for cp in left:
                cp().start()

        @pl.when(w < NW - 1)
        def _():
            for cp in right:
                cp().start()

    sub = lax.broadcasted_iota(jnp.int32, (TB, C), 0)

    def put(u, r, lo, hi):
        b0 = u[r, :TB, :].astype(F32)
        u[r, :TB, :] = jnp.where(sub == 0, lo, b0).astype(BF16)
        b1 = u[r, TW + TB:, :].astype(F32)
        u[r, TW + TB:, :] = jnp.where(sub == TB - 1, hi, b1).astype(BF16)

    def halo_row(q, u):
        halo_copies(q, u)[0]().wait()

    def halo_cols(q, u):
        _, left, right = halo_copies(q, u)

        @pl.when(w > 0)
        def _():
            for cp in left:
                cp().wait_send()
            for cp in right:
                cp().wait_recv()

        @pl.when(w < NW - 1)
        def _():
            for cp in right:
                cp().wait_send()
            for cp in left:
                cp().wait_recv()

        def step(k):
            for i in range(4):
                r = k * 4 + i
                put(u, r + 1, cr[q, 0, pl.ds(r, 1), :], cr[q, 1, pl.ds(r, 1), :])
        _loop(0, TH // 4, step)
        put(u, 33 * (1 - h), cc[q, 0, pl.ds(7 * h, 1), :], cc[q, 1, pl.ds(7 * h, 1), :])

    def permute_in(q, src, u):
        for k in range(NX):
            if q == 1:
                loads[q, k].wait()

            def step(i):
                for d in range(16):
                    r = k * rows + i * 16 + d
                    v = jnp.dot(pm[:, :], src[r], preferred_element_type=F32)
                    u[r + 1] = v.astype(BF16)
                    if q == 1:
                        cs[q, 0, pl.ds(r, 1), :] = v[TB:TB + 1]
                        cs[q, 1, pl.ds(r, 1), :] = v[TW + TB - 1:TW + TB]
            _loop(0, rows // 16, step)

    def pad_blocks(q, u, r, first, last):
        u[r + 1, :TB, :] = jnp.where(sub == 0, 0.0, pltpu.roll(last, 1, 0)).astype(BF16)
        u[r + 1, TW + TB:, :] = jnp.where(sub == TB - 1, 0.0, pltpu.roll(first, TB - 1, 0)).astype(BF16)
        cs[q, 0, pl.ds(r, 1), :] = first[0:1]
        cs[q, 1, pl.ds(r, 1), :] = last[TB - 1:TB]

    def conv(u, wt, r0, R=R):
        lhs = jnp.concatenate([u[pl.ds(r0 + a, R), TB * b:TB * b + TW, :].reshape(R * TW, C) for a in range(3) for b in range(3)], axis=1)
        return jnp.dot(lhs, wt[:, :], preferred_element_type=F32)

    def stat_copies(q):
        out = []
        for k in range(1, ND):
            t = lax.rem(me + k, ND)
            out.append(rcopy(stat.at[q, me], stat.at[q, me], st_send.at[q], st_recv.at[q], {"w": t // NH, "h": lax.rem(t, NH)}))
        return out

    def stat_start(q, a, b):
        stat[q, me] = jnp.concatenate([a, b, jnp.zeros((6, C), F32)], axis=0)
        for cp in stat_copies(q):
            cp.start()

    def stat_finish(q):
        others = stat.at[q, pl.ds(0, ND - 1)]
        rcopy(others, others, st_send.at[q], st_recv.at[q], dev_c).wait()
        tot = stat[q, 0]
        for k in range(1, ND):
            tot = tot + stat[q, k]
        return tot

    xb = lax.rem(w, 2)
    yb = w // 2
    dev_x = {"w": w + 1 - 2 * xb, "h": h}
    dev_y = {"w": w + 2 - 4 * yb, "h": h}
    dev_c = {"w": w, "h": 1 - h}

    BS = (1, 0, 2)

    def part(n, c, off, size):
        return dw.at[n, c, :, pl.ds(pl.multiple_of(off, 16), size), :]

    def half(n, c, off, size):
        return rd.at[n, c, :, pl.ds(pl.multiple_of(off, 16), size), :]

    def ar_copies(n, c):
        mine, other = 128 * h, 128 * (1 - h)
        o0, o1 = 32 * xb + 16 * yb, 64 + 32 * yb + 16 * xb
        q0, q1 = 32 * xb, 64 + 32 * yb
        out = (dw2_hbm, dw1_hbm)[n].at[:, BS[c], pl.ds(pl.multiple_of(mine, 128), 128), :]
        plan = (
            (part(n, c, other, 128), rd.at[n, c], dev_c),
            (part(n, c, mine + 32 * (1 - xb), 32), r1.at[n, c, 0], dev_x),
            (part(n, c, mine + 64 + 32 * (1 - yb), 32), r1.at[n, c, 1], dev_y),
            (part(n, c, mine + 32 * xb + 16 * (1 - yb), 16), r2.at[n, c, 0], dev_y),
            (part(n, c, mine + 64 + 32 * yb + 16 * (1 - xb), 16), r2.at[n, c, 1], dev_x),
            (half(n, c, o0, 16), half(n, c, o0, 16), dev_y),
            (half(n, c, o1, 16), half(n, c, o1, 16), dev_x),
            (half(n, c, q0, 32), half(n, c, q0, 32), dev_x),
            (half(n, c, q1, 32), half(n, c, q1, 32), dev_y),
            (rd.at[n, c], out, dev_c),
        )

        def make(k):
            src, dst, dev = plan[k]
            return lambda: rcopy(src, dst, ar_send.at[n, c, k % 2], ar_recv.at[n, c, k], dev)
        return [make(k) for k in range(10)] + [lambda: pltpu.make_async_copy(rd.at[n, c], out, in_sem.at[n * 3 + c])]

    AR_SETS = ((0,), (1, 2), (3, 4), (5, 6), (7, 8), (9, 10))

    def accumulate(n, c, off, size, src, into=None):
        sl = pl.ds(pl.multiple_of(128 * h + off, 16), size)
        for t in range(3):
            v = dw[n, c, t, sl, :] + src[t]
            if into is None:
                dw[n, c, t, sl, :] = v
            else:
                rd[n, c, t, pl.ds(pl.multiple_of(off, 16), size), :] = v

    def ar_step(n, c, k):
        with jax.named_scope(f"ar_{n}_{c}_{k}"):
            cps = ar_copies(n, c)
            if k > 0:
                for i in AR_SETS[k - 1]:
                    cps[i]().wait()
            if k == 1:
                accumulate(n, c, 0, 128, rd.at[n, c])
            if k == 2:
                accumulate(n, c, 32 * xb, 32, r1.at[n, c, 0])
                accumulate(n, c, 64 + 32 * yb, 32, r1.at[n, c, 1])
            if k == 3:
                accumulate(n, c, 32 * xb + 16 * yb, 16, r2.at[n, c, 0], rd)
                accumulate(n, c, 64 + 32 * yb + 16 * xb, 16, r2.at[n, c, 1], rd)
            if k < 6:
                for i in AR_SETS[k]:
                    cps[i]().start()

    SLOTS = "347:?FI79<@CKQ:;>AHNQ@BGJMQRCEILNRREFILORR"
    plan_at = {}
    for i_, ch_ in enumerate(SLOTS):
        plan_at.setdefault(ord(ch_) - ord("0"), []).append((i_ // 21, i_ // 7 % 3, i_ % 7))

    def sums_at(base, lo, hi, i):
        for sl in range(lo, hi):
            if sl + base in plan_at:
                def _(todo=plan_at[sl + base]):
                    for n, c, k in sorted(todo, key=lambda e: -e[2]):
                        ar_step(n, c, k)
                pl.when(i == sl)(_)

    def perm3(i):
        return (3 * i * i - 5 * i + 2) // 2

    def turn(n, t):
        dw[n, t // 3, perm3(t % 3)] = raw[:, :].T

    def tap(n, u, vt, t, first):
        turn(n, lax.max(t - 1, first))
        rhs = u[pl.ds(perm3(t % 3), TH), pl.ds(pl.multiple_of(TB * perm3(t // 3), TB), TW), :].reshape(TH * TW, C)
        lhs = jnp.concatenate([vt[r] for r in range(TH)], axis=1)
        raw[:, :] = jnp.dot(lhs, rhs, preferred_element_type=F32)

    def x_edges(i):
        for d in range(8):
            r = i * 8 + d
            cs[0, 0, pl.ds(r, 1), :] = xn[r, :TB, :].astype(F32)[:1]
            cs[0, 1, pl.ds(r, 1), :] = xn[r, TW - TB:, :].astype(F32)[TB - 1:]
    with jax.named_scope("edges"):
        for k in range(NX):
            loads[0, k].wait()
        _loop(0, TH // 8, x_edges)
    with jax.named_scope("barrier"):
        pl.semaphore_wait(barrier, ND - 1)
    halo_start(0, ux, False)
    with jax.named_scope("perm_x"):
        permute_in(0, xn, ux)
    halo_copies(0, ux)[0]().start()
    with jax.named_scope("perm_g"):
        permute_in(1, gn, ug)
    halo_start(1, ug)
    loads[0, "w"].wait()
    loads[1, "w"].wait()
    with jax.named_scope("hfin_x"):
        halo_row(0, ux)
        halo_cols(0, ux)

    def wtrans(k):
        for i in range(3):
            t = lax.min(k * 3 + i, 8)
            src, dst = pl.ds(pl.multiple_of(t * C, C), C), pl.ds(pl.multiple_of((8 - t) * C, C), C)
            w1t[dst, :] = w1[src, :].T
            w2t[dst, :] = w2[src, :].T

    def conv1_step(k, carry):
        s1, s2 = carry
        wtrans(k)
        a = conv(ux, w1, k * 8, 8).astype(BF16)
        abuf[pl.ds(k * 8, 8)] = a.reshape(8, TW, C)
        af = a.astype(F32)
        return s1 + _fold8(af), s2 + _fold8(af * af)
    zero = jnp.zeros((8, C), F32)
    with jax.named_scope("conv1"):
        s1, s2 = lax.fori_loop(0, TH // 8, conv1_step, (zero, zero))
    with jax.named_scope("ststart"):
        stat_start(0, _row(s1), _row(s2))
    with jax.named_scope("hfin_g"):
        halo_row(1, ug)
        halo_cols(1, ug)

    def convt2(k, R=R):
        dz[pl.ds(k * R, R)] = conv(ug, w2t, k * R, R).reshape(R, TW, C)
        for i in range(R):
            r = k * R + i
            gn[r] = ug[r + 1, TB:TB + TW, :].T
    with jax.named_scope("convt2"):
        _loop(0, 2, lambda k: convt2(k, 2 * R))

    with jax.named_scope("stat0"):
        tot = _group_sum(stat_finish(0)) / CNT
    mean = tot[0:1]
    rstd = lax.rsqrt(tot[1:2] - mean * mean + EPS)
    loads[0, "v"].wait()
    loads[1, "v"].wait()
    gam = vec[0]
    bet = vec[1]
    ngain = rstd * gam

    SB = TB

    def gate(r, sl):
        am = abuf[r, sl, :].astype(F32) - mean
        n = am * ngain + bet
        n2 = n * n
        th = jnp.tanh(n * (n2 * (GC0 * GC1) + GC0))
        return am, n, n2, 0.5 * th + 0.5

    def slope(n, n2, hp):
        return hp + n * ((hp - hp * hp) * (n2 * (6.0 * GC0 * GC1) + 2.0 * GC0))

    def act_row(r, carry, do_z, do_dn):
        t0, t1 = carry
        first = last = None
        for i in range(TW // SB):
            sl = pl.ds(i * SB, SB)
            am, n, n2, hp = gate(r, sl)
            if do_z:
                z = n * hp
                uz[r + 1, pl.ds(TB + i * SB, SB), :] = z.astype(BF16)
                first = z[:TB] if first is None else first
                last = z[SB - TB:]
            if do_dn:
                dn = dz[r, sl, :] * slope(n, n2, hp)
                dz[r, sl, :] = dn
                t0 = t0 + _fold8(dn * am)
                t1 = t1 + _fold8(dn)
        if do_z:
            pad_blocks(2, uz, r, first, last)
        return t0, t1

    def convt2_z(k):
        with jax.named_scope("convt2z"):
            for i in range(8):
                act_row((k - 4) * 8 + i, (zero, zero), True, False)
            convt2(k)
    _loop(4, 8, convt2_z)
    with jax.named_scope("hstart"):
        halo_start(2, uz)
    raw[:, :] = jnp.zeros((C, C), F32)

    def tap2(lo, hi, first, rows, carry):
        def step(t, c):
            sums_at(0, lo, hi, t)
            if lo == 0:
                @pl.when(t == 1)
                def _():
                    with jax.named_scope("hrow_z"):
                        halo_row(2, uz)
            with jax.named_scope("tap2"):
                for i in range(rows):
                    c = act_row((t - lo) * rows + i, c, False, True)
                tap(0, uz, gn, t, first)
            return c
        return lax.fori_loop(lo, hi, step, carry)

    sums = tap2(0, 3, 0, 0, (zero, zero))
    turn(0, 2)
    with jax.named_scope("hcol_z"):
        halo_cols(2, uz)
    sums = tap2(3, 7, 3, 8, sums)
    with jax.named_scope("ststart"):
        stat_start(1, _row(sums[0]) * rstd, _row(sums[1]))
    tap2(7, 9, 3, 0, zero)
    turn(0, 8)

    def out_copy(q, k):
        src, dst = (ost if q == 0 else abuf, (y_hbm, dx_hbm)[q])
        return pltpu.make_async_copy(src.at[pl.ds(k * R, R)], dst.at[pl.ds(k * R, R)], out_sem.at[q])

    def out_step(q, u, wt, res, out, k):
        acc = conv(u, wt, k * R).reshape(R, TW, C)
        v = acc + res[pl.ds(k * R + 1, R), TB:TB + TW, :].astype(F32)
        out[pl.ds(k * R, R)] = v.astype(BF16)
        out_copy(q, k).start()

    def y_rows(lo, hi, slot, extra=None):
        def step(k):
            sums_at(slot - lo, lo, hi, k)
            with jax.named_scope("y"):
                if extra is not None:
                    extra(k)
                out_step(0, uz, w2, ux, ost, k)
        _loop(lo, hi, step)
    y_rows(0, 1, 9)

    with jax.named_scope("stat1"):
        tot = stat_finish(1)
    vec[2] = tot[0:1]
    vec[3] = tot[1:2]
    outv = [pltpu.make_async_copy(vec.at[2 + q], (dgam_hbm, dbet_hbm)[q], vec_sem.at[q]) for q in range(2)]
    for cp in outv:
        cp.start()
    us = _group_sum(tot * gam) / CNT
    k0 = rstd * gam
    k1 = rstd * rstd * us[0:1]
    k2 = rstd * us[1:2]

    def da_row(r):
        first = last = None
        for i in range(TW // SB):
            sl = pl.ds(i * SB, SB)
            am = abuf[r, sl, :].astype(F32) - mean
            d = dz[r, sl, :] * k0 - (am * k1 + k2)
            ud[r + 1, pl.ds(TB + i * SB, SB), :] = d.astype(BF16)
            first = d[:TB] if first is None else first
            last = d[SB - TB:]
        pad_blocks(3, ud, r, first, last)
        xn[r] = ud[r + 1, TB:TB + TW, :].T

    def da_rows(k):
        for i in range(16):
            da_row((k - 1) * 16 + i)
    y_rows(1, 3, 10, da_rows)
    with jax.named_scope("hstart"):
        halo_start(3, ud)

    def wgrad1_step(t):
        sums_at(12, 0, 9, t)
        with jax.named_scope("tap1"):
            tap(1, ux, xn, t, 0)
    _loop(0, 9, wgrad1_step)
    turn(1, 8)
    with jax.named_scope("hfin_d"):
        halo_row(3, ud)
        halo_cols(3, ud)

    def dx_step(k):
        sums_at(21, 0, 8, k)
        with jax.named_scope("dx"):
            out_step(1, ud, w1t, ug, abuf, k)

    _loop(0, TH // R, dx_step)
    y_rows(3, 8, 29)
    for n, c, k in sorted(plan_at[34], key=lambda e: e[2]):
        ar_step(n, c, k)
    with jax.named_scope("outw"):
        for q in range(2):
            outv[q].wait()
            src, dst = (ost if q == 0 else abuf, (y_hbm, dx_hbm)[q])
            pltpu.make_async_copy(src, dst, out_sem.at[q]).wait()


def finish(y_ref, dx_ref, w1_ref, w2_ref, ga_ref, be_ref, yo, dxo, w1o, w2o, gao, beo,
           yi, dxi, yb, dxb, w1b, w2b, gab, beb, qm, isem, osem):
    nc = 2
    n = TH // nc
    jobs = []
    for k in range(nc):
        part = pl.ds(k * n, n)
        for src, mid, buf, dst in ((dx_ref, dxi, dxb, dxo), (y_ref, yi, yb, yo)):
            jobs.append((src.at[part], mid.at[part], buf.at[part], dst.at[part]))
        src, buf, dst = ((w2_ref, w2b, w2o), (w1_ref, w1b, w1o))[k]
        jobs.append((src, buf, None, dst))
    jobs += [(ga_ref, gab, None, gao), (be_ref, beb, None, beo)]
    ins = [pltpu.make_async_copy(src, mid, isem.at[i]) for i, (src, mid, _, _) in enumerate(jobs)]
    for cp in ins:
        cp.start()
    qi = lax.broadcasted_iota(jnp.int32, (TW, TW), 0)
    qj = lax.broadcasted_iota(jnp.int32, (TW, TW), 1)
    qm[:, :] = jnp.where(qi == (qj & 15) * TB + (qj >> 4), 1.0, 0.0).astype(BF16)
    outs = []
    for i, (_, mid, buf, dst) in enumerate(jobs):
        ins[i].wait()
        if buf is not None:
            for r in range(n):
                buf[r] = jnp.dot(qm[:, :], mid[r], preferred_element_type=F32).astype(BF16)
        outs.append(pltpu.make_async_copy(mid if buf is None else buf, dst, osem.at[i]))
        outs[i].start()
    for cp in outs:
        cp.wait()


def solution(mesh):
    tile = P(None, 'h', 'w', None)

    def body(x, w1, gamma, beta, w2, g):
        anyspec = pl.BlockSpec(memory_space=pl.ANY)
        S = jax.ShapeDtypeStruct
        V = pltpu.VMEM
        DMA = pltpu.SemaphoreType.DMA
        img = (TH, TW, C)
        uimg = (TH + 2, EXT, C)
        out = pl.pallas_call(
            kernel,
            out_shape=(S(img, BF16), S(img, BF16), S((3, 3, C, C), F32), S((3, 3, C, C), F32), S((1, C), F32), S((1, C), F32)),
            in_specs=[anyspec] * 6,
            out_specs=(anyspec,) * 6,
            scratch_shapes=[
                V(img, BF16), V(img, BF16), V(uimg, BF16), V(uimg, BF16), V(uimg, BF16), V(uimg, BF16),
                V(img, BF16), V(img, BF16), V(img, F32), V((C, C), F32),
                V((9 * C, C), BF16), V((9 * C, C), BF16), V((9 * C, C), BF16), V((9 * C, C), BF16),
                V((2, 3, 3, C, C), F32), V((2, 3, 3, 128, C), F32), V((2, 3, 2, 3, 32, C), F32), V((2, 3, 2, 3, 16, C), F32),
                V((4, 2, TH, C), F32), V((4, 2, TH, C), F32), V((4, 2, 8, C), F32), V((2, ND, 8, C), F32),
                V((EXT, TW), BF16), V((4, 1, C), F32),
                DMA((2 * NX + 2,)), DMA((2,)), DMA((2,)), DMA((4, 5)), DMA((4, 5)), DMA((2,)), DMA((2,)), DMA((2, 3, 2)), DMA((2, 3, 10)),
            ],
            compiler_params=pltpu.CompilerParams(collective_id=0, has_side_effects=True, vmem_limit_bytes=67043328),
        )(x.reshape(img), w1.reshape(9 * C, C), gamma.reshape(1, C), beta.reshape(1, C), w2.reshape(9 * C, C), g.reshape(img))
        y, dx, dw1, dw2, dgam, dbet = out
        wgt = (9 * C, C)
        row = (1, C)
        shapes = [S(img, BF16), S(img, BF16), S(wgt, F32), S(wgt, F32), S(row, F32), S(row, F32)]
        y, dx, dw1, dw2, dgam, dbet = pl.pallas_call(
            finish,
            out_shape=tuple(shapes),
            in_specs=[anyspec] * 6,
            out_specs=(anyspec,) * 6,
            scratch_shapes=[V(img, BF16), V(img, BF16)] + [V(o.shape, o.dtype) for o in shapes] + [V((TW, TW), BF16), DMA((8,)), DMA((8,))],
            compiler_params=pltpu.CompilerParams(vmem_limit_bytes=67043328),
        )(y, dx, dw1.reshape(wgt), dw2.reshape(wgt), dgam, dbet)
        return (y.reshape(x.shape), dx.reshape(x.shape), dw1.reshape(w1.shape), dw2.reshape(w2.shape), dgam.reshape(C), dbet.reshape(C))

    return jax.shard_map(body, mesh=mesh, in_specs=(tile, P(), P(), P(), P(), tile), out_specs=(tile, tile, P(), P(), P(), P()), check_vma=False)
```

```python
import functools

import jax
import jax.numpy as jnp
from jax import lax
from jax.experimental import pallas as pl
from jax.experimental.pallas import tpu as pltpu
from jax.sharding import PartitionSpec as P

GROUPS = 32
EPS = 1e-5
MESH = pl.DeviceIdType.MESH
F32 = jnp.float32
BF16 = jnp.bfloat16
GC0 = 0.7978845608028654
GC1 = 0.044715
TH, TW, C = 32, 256, 256
CG = C // GROUPS
NW, NH = 4, 2
ND = NW * NH
CNT = float(TH * NH * TW * NW * CG)
TB = 16
EXT = TW + 2 * TB
R = 4
NX = 2


def _group_sum(v):
    lane = lax.broadcasted_iota(jnp.int32, v.shape, 1)
    for k in (1, 2, 4):
        up = pltpu.roll(v, C - k, 1)
        down = pltpu.roll(v, k, 1)
        v = v + jnp.where((lane & k) == 0, up, down)
    return v


def _loop(lo, hi, f):
    def body(i, c):
        f(i)
        return c
    lax.fori_loop(lo, hi, body, 0)


def _row(v):
    return v.sum(0, keepdims=True)


def _fold8(v):
    return v.reshape(v.shape[0] // 8, 8, C).sum(0)


def kernel(x_hbm, w1_hbm, gam_hbm, bet_hbm, w2_hbm, g_hbm,
           y_hbm, dx_hbm, dw1_hbm, dw2_hbm, dgam_hbm, dbet_hbm,
           xn, gn, ux, ug, uz, ud, abuf, ost, dz, raw, w1, w2, w1t, w2t, dw, rd, r1, r2,
           cs, cr, cc, stat, pm, vec,
           in_sem, vec_sem, out_sem, hs_send, hs_recv, st_send, st_recv, ar_send, ar_recv):
    w = lax.axis_index("w")
    h = lax.axis_index("h")
    me = w * NH + h

    rows = TH // NX
    loads = {}
    for q, (src, dst) in enumerate(((x_hbm, xn), (g_hbm, gn))):
        for k in range(NX):
            cp = pltpu.make_async_copy(src.at[pl.ds(k * rows, rows)], dst.at[pl.ds(k * rows, rows)], in_sem.at[q * NX + k])
            cp.start()
            loads[q, k] = cp
        wsrc, wdst = ((w1_hbm, w1), (w2_hbm, w2))[q]
        cp = pltpu.make_async_copy(wsrc, wdst, in_sem.at[2 * NX + q])
        cp.start()
        loads[q, "w"] = cp
        cp = pltpu.make_async_copy((gam_hbm, bet_hbm)[q], vec.at[q], vec_sem.at[q])
        cp.start()
        loads[q, "v"] = cp

    barrier = pltpu.get_barrier_semaphore()
    for k in range(1, ND):
        t = lax.rem(me + k, ND)
        pl.semaphore_signal(barrier, inc=1, device_id={"w": t // NH, "h": lax.rem(t, NH)}, device_id_type=MESH)

    pi = lax.broadcasted_iota(jnp.int32, (EXT, TW), 0)
    pj = lax.broadcasted_iota(jnp.int32, (EXT, TW), 1)
    pm[:, :] = jnp.where(pj == (pi & 15) * TB + (pi >> 4) - 1, 1.0, 0.0).astype(BF16)
    for u in (ux, ug, uz, ud):
        u[pl.ds(33 * h, 1)] = jnp.zeros((1, EXT, C), BF16)

    def no_neighbour(side):
        cr[:, side] = jnp.zeros((4, TH, C), F32)
        cc[:, side] = jnp.zeros((4, 8, C), F32)
    pl.when(w == 0)(lambda: no_neighbour(0))
    pl.when(w == NW - 1)(lambda: no_neighbour(1))

    def to_dev(dw_, dh):
        return {"w": w + dw_, "h": h if dh == 0 else 1 - h}

    def rcopy(src, dst, ss, rs, dev):
        return pltpu.make_async_remote_copy(src_ref=src, dst_ref=dst, send_sem=ss, recv_sem=rs, device_id=dev, device_id_type=MESH)

    def halo_copies(q, u):
        slab = pl.ds(pl.multiple_of(24 * (1 - h), 8), 8)

        def make(m, src, dst, dev):
            return lambda: rcopy(src, dst, hs_send.at[q, m], hs_recv.at[q, m], dev)
        row = make(0, u.at[pl.ds(32 - 31 * h, 1)], u.at[pl.ds(33 * h, 1)], to_dev(0, 1))
        left = [make(1, cs.at[q, 0], cr.at[q, 1], to_dev(-1, 0)), make(2, cs.at[q, 0, slab], cc.at[q, 1], to_dev(-1, 1))]
        right = [make(3, cs.at[q, 1], cr.at[q, 0], to_dev(1, 0)), make(4, cs.at[q, 1, slab], cc.at[q, 0], to_dev(1, 1))]
        return row, left, right

    def halo_start(q, u, row_too=True):
        row, left, right = halo_copies(q, u)
        if row_too:
            row().start()

        @pl.when(w > 0)
        def _():
            for cp in left:
                cp().start()

        @pl.when(w < NW - 1)
        def _():
            for cp in right:
                cp().start()

    sub = lax.broadcasted_iota(jnp.int32, (TB, C), 0)

    def put(u, r, lo, hi):
        b0 = u[r, :TB, :].astype(F32)
        u[r, :TB, :] = jnp.where(sub == 0, lo, b0).astype(BF16)
        b1 = u[r, TW + TB:, :].astype(F32)
        u[r, TW + TB:, :] = jnp.where(sub == TB - 1, hi, b1).astype(BF16)

    def halo_row(q, u):
        halo_copies(q, u)[0]().wait()

    def halo_cols(q, u):
        _, left, right = halo_copies(q, u)

        @pl.when(w > 0)
        def _():
            for cp in left:
                cp().wait_send()
            for cp in right:
                cp().wait_recv()

        @pl.when(w < NW - 1)
        def _():
            for cp in right:
                cp().wait_send()
            for cp in left:
                cp().wait_recv()

        def step(k):
            for i in range(8):
                r = k * 8 + i
                put(u, r + 1, cr[q, 0, pl.ds(r, 1), :], cr[q, 1, pl.ds(r, 1), :])
        _loop(0, TH // 8, step)
        put(u, 33 * (1 - h), cc[q, 0, pl.ds(7 * h, 1), :], cc[q, 1, pl.ds(7 * h, 1), :])

    def permute_in(q, src, u):
        for k in range(NX):
            if q == 1:
                loads[q, k].wait()

            def step(i):
                for d in range(16):
                    r = k * rows + i * 16 + d
                    v = jnp.dot(pm[:, :], src[r], preferred_element_type=F32)
                    u[r + 1] = v.astype(BF16)
                    if q == 1:
                        cs[q, 0, pl.ds(r, 1), :] = v[TB:TB + 1]
                        cs[q, 1, pl.ds(r, 1), :] = v[TW + TB - 1:TW + TB]
            _loop(0, rows // 16, step)

    def pad_blocks(q, u, r, first, last):
        u[r + 1, :TB, :] = jnp.where(sub == 0, 0.0, pltpu.roll(last, 1, 0)).astype(BF16)
        u[r + 1, TW + TB:, :] = jnp.where(sub == TB - 1, 0.0, pltpu.roll(first, TB - 1, 0)).astype(BF16)
        cs[q, 0, pl.ds(r, 1), :] = first[0:1]
        cs[q, 1, pl.ds(r, 1), :] = last[TB - 1:TB]

    def conv(u, wt, r0, R=R):
        lhs = jnp.concatenate([u[pl.ds(r0 + a, R), TB * b:TB * b + TW, :].reshape(R * TW, C) for a in range(3) for b in range(3)], axis=1)
        return jnp.dot(lhs, wt[:, :], preferred_element_type=F32)

    def stat_copies(q):
        out = []
        for k in range(1, ND):
            t = lax.rem(me + k, ND)
            out.append(rcopy(stat.at[q, me], stat.at[q, me], st_send.at[q], st_recv.at[q], {"w": t // NH, "h": lax.rem(t, NH)}))
        return out

    def stat_start(q, a, b):
        stat[q, me] = jnp.concatenate([a, b, jnp.zeros((6, C), F32)], axis=0)
        for cp in stat_copies(q):
            cp.start()

    def stat_finish(q):
        others = stat.at[q, pl.ds(0, ND - 1)]
        rcopy(others, others, st_send.at[q], st_recv.at[q], dev_c).wait()
        tot = stat[q, 0]
        for k in range(1, ND):
            tot = tot + stat[q, k]
        return tot

    xb = lax.rem(w, 2)
    yb = w // 2
    dev_x = {"w": w + 1 - 2 * xb, "h": h}
    dev_y = {"w": w + 2 - 4 * yb, "h": h}
    dev_c = {"w": w, "h": 1 - h}

    BS = (1, 0, 2)

    def part(n, c, off, size):
        return dw.at[n, c, :, pl.ds(pl.multiple_of(off, 16), size), :]

    def half(n, c, off, size):
        return rd.at[n, c, :, pl.ds(pl.multiple_of(off, 16), size), :]

    def ar_copies(n, c):
        mine, other = 128 * h, 128 * (1 - h)
        o0, o1 = 32 * xb + 16 * yb, 64 + 32 * yb + 16 * xb
        q0, q1 = 32 * xb, 64 + 32 * yb
        out = (dw2_hbm, dw1_hbm)[n].at[:, BS[c], pl.ds(pl.multiple_of(mine, 128), 128), :]
        plan = (
            (part(n, c, other, 128), rd.at[n, c], dev_c),
            (part(n, c, mine + 32 * (1 - xb), 32), r1.at[n, c, 0], dev_x),
            (part(n, c, mine + 64 + 32 * (1 - yb), 32), r1.at[n, c, 1], dev_y),
            (part(n, c, mine + 32 * xb + 16 * (1 - yb), 16), r2.at[n, c, 0], dev_y),
            (part(n, c, mine + 64 + 32 * yb + 16 * (1 - xb), 16), r2.at[n, c, 1], dev_x),
            (half(n, c, o0, 16), half(n, c, o0, 16), dev_y),
            (half(n, c, o1, 16), half(n, c, o1, 16), dev_x),
            (half(n, c, q0, 32), half(n, c, q0, 32), dev_x),
            (half(n, c, q1, 32), half(n, c, q1, 32), dev_y),
            (rd.at[n, c], out, dev_c),
        )

        def make(k):
            src, dst, dev = plan[k]
            return lambda: rcopy(src, dst, ar_send.at[n, c, k % 2], ar_recv.at[n, c, k], dev)
        return [make(k) for k in range(10)] + [lambda: pltpu.make_async_copy(rd.at[n, c], out, in_sem.at[n * 3 + c])]

    AR_SETS = ((0,), (1, 2), (3, 4), (5, 6), (7, 8), (9, 10))

    def accumulate(n, c, off, size, src, into=None):
        sl = pl.ds(pl.multiple_of(128 * h + off, 16), size)
        for t in range(3):
            v = dw[n, c, t, sl, :] + src[t]
            if into is None:
                dw[n, c, t, sl, :] = v
            else:
                rd[n, c, t, pl.ds(pl.multiple_of(off, 16), size), :] = v

    def ar_step(n, c, k):
        with jax.named_scope(f"ar_{n}_{c}_{k}"):
            cps = ar_copies(n, c)
            if k > 0:
                for i in AR_SETS[k - 1]:
                    cps[i]().wait()
            if k == 1:
                accumulate(n, c, 0, 128, rd.at[n, c])
            if k == 2:
                accumulate(n, c, 32 * xb, 32, r1.at[n, c, 0])
                accumulate(n, c, 64 + 32 * yb, 32, r1.at[n, c, 1])
            if k == 3:
                accumulate(n, c, 32 * xb + 16 * yb, 16, r2.at[n, c, 0], rd)
                accumulate(n, c, 64 + 32 * yb + 16 * xb, 16, r2.at[n, c, 1], rd)
            if k < 6:
                for i in AR_SETS[k]:
                    cps[i]().start()

    SLOTS = "347:?FI79<@CKQ:;>AHNQ@BGJMQRCEILNRREFILORR"
    plan_at = {}
    for i_, ch_ in enumerate(SLOTS):
        plan_at.setdefault(ord(ch_) - ord("0"), []).append((i_ // 21, i_ // 7 % 3, i_ % 7))

    def sums_at(base, lo, hi, i):
        for sl in range(lo, hi):
            if sl + base in plan_at:
                def _(todo=plan_at[sl + base]):
                    for n, c, k in sorted(todo, key=lambda e: -e[2]):
                        ar_step(n, c, k)
                pl.when(i == sl)(_)

    def perm3(i):
        return (3 * i * i - 5 * i + 2) // 2

    def turn(n, t):
        dw[n, t // 3, perm3(t % 3)] = raw[:, :].T

    def tap(n, u, vt, t, first):
        turn(n, lax.max(t - 1, first))
        rhs = u[pl.ds(perm3(t % 3), TH), pl.ds(pl.multiple_of(TB * perm3(t // 3), TB), TW), :].reshape(TH * TW, C)
        lhs = jnp.concatenate([vt[r] for r in range(TH)], axis=1)
        raw[:, :] = jnp.dot(lhs, rhs, preferred_element_type=F32)

    def x_edges(i):
        for d in range(16):
            r = i * 16 + d
            cs[0, 0, pl.ds(r, 1), :] = xn[r, :TB, :].astype(F32)[:1]
            cs[0, 1, pl.ds(r, 1), :] = xn[r, TW - TB:, :].astype(F32)[TB - 1:]
    with jax.named_scope("edges"):
        for k in range(NX):
            loads[0, k].wait()
        _loop(0, TH // 16, x_edges)
    with jax.named_scope("barrier"):
        pl.semaphore_wait(barrier, ND - 1)
    halo_start(0, ux, False)
    with jax.named_scope("perm_x"):
        permute_in(0, xn, ux)
    halo_copies(0, ux)[0]().start()
    with jax.named_scope("perm_g"):
        permute_in(1, gn, ug)
    halo_start(1, ug)
    loads[0, "w"].wait()
    loads[1, "w"].wait()
    with jax.named_scope("hfin_x"):
        halo_row(0, ux)
        halo_cols(0, ux)

    def wtrans(k):
        for i in range(3):
            t = lax.min(k * 3 + i, 8)
            src, dst = pl.ds(pl.multiple_of(t * C, C), C), pl.ds(pl.multiple_of((8 - t) * C, C), C)
            w1t[dst, :] = w1[src, :].T
            w2t[dst, :] = w2[src, :].T

    def conv1_step(k, carry):
        s1, s2 = carry
        wtrans(k)
        a = conv(ux, w1, k * 8, 8).astype(BF16)
        abuf[pl.ds(k * 8, 8)] = a.reshape(8, TW, C)
        af = a.astype(F32)
        return s1 + _fold8(af), s2 + _fold8(af * af)
    zero = jnp.zeros((8, C), F32)
    with jax.named_scope("conv1"):
        s1, s2 = lax.fori_loop(0, TH // 8, conv1_step, (zero, zero))
    with jax.named_scope("ststart"):
        stat_start(0, _row(s1), _row(s2))
    with jax.named_scope("hfin_g"):
        halo_row(1, ug)
        halo_cols(1, ug)

    def convt2(k, R=R):
        dz[pl.ds(k * R, R)] = conv(ug, w2t, k * R, R).reshape(R, TW, C)
        for i in range(R):
            r = k * R + i
            gn[r] = ug[r + 1, TB:TB + TW, :].T
    with jax.named_scope("convt2"):
        _loop(0, 2, lambda k: convt2(k, 2 * R))

    with jax.named_scope("stat0"):
        tot = _group_sum(stat_finish(0)) / CNT
    mean = tot[0:1]
    rstd = lax.rsqrt(tot[1:2] - mean * mean + EPS)
    loads[0, "v"].wait()
    loads[1, "v"].wait()
    gam = vec[0]
    bet = vec[1]
    ngain = rstd * gam

    SB = TB

    def gate(r, sl):
        am = abuf[r, sl, :].astype(F32) - mean
        n = am * ngain + bet
        n2 = n * n
        th = jnp.tanh(n * (n2 * (GC0 * GC1) + GC0))
        return am, n, n2, 0.5 * th + 0.5

    def slope(n, n2, hp):
        return hp + n * ((hp - hp * hp) * (n2 * (6.0 * GC0 * GC1) + 2.0 * GC0))

    def act_row(r, carry, do_z, do_dn):
        t0, t1 = carry
        first = last = None
        for i in range(TW // SB):
            sl = pl.ds(i * SB, SB)
            am, n, n2, hp = gate(r, sl)
            if do_z:
                z = n * hp
                uz[r + 1, pl.ds(TB + i * SB, SB), :] = z.astype(BF16)
                first = z[:TB] if first is None else first
                last = z[SB - TB:]
            if do_dn:
                dn = dz[r, sl, :] * slope(n, n2, hp)
                dz[r, sl, :] = dn
                t0 = t0 + _fold8(dn * am)
                t1 = t1 + _fold8(dn)
        if do_z:
            pad_blocks(2, uz, r, first, last)
        return t0, t1

    def convt2_z(k):
        with jax.named_scope("convt2z"):
            for i in range(8):
                act_row((k - 4) * 8 + i, (zero, zero), True, False)
            convt2(k)
    _loop(4, 8, convt2_z)
    with jax.named_scope("hstart"):
        halo_start(2, uz)
    raw[:, :] = jnp.zeros((C, C), F32)

    def tap2(lo, hi, first, rows, carry):
        def step(t, c):
            sums_at(0, lo, hi, t)
            if lo == 0:
                @pl.when(t == 1)
                def _():
                    with jax.named_scope("hrow_z"):
                        halo_row(2, uz)
            with jax.named_scope("tap2"):
                for i in range(rows):
                    c = act_row((t - lo) * rows + i, c, False, True)
                tap(0, uz, gn, t, first)
            return c
        return lax.fori_loop(lo, hi, step, carry)

    sums = tap2(0, 3, 0, 0, (zero, zero))
    turn(0, 2)
    with jax.named_scope("hcol_z"):
        halo_cols(2, uz)
    sums = tap2(3, 7, 3, 8, sums)
    with jax.named_scope("ststart"):
        stat_start(1, _row(sums[0]) * rstd, _row(sums[1]))
    tap2(7, 9, 3, 0, zero)
    turn(0, 8)

    def out_copy(q, k):
        src, dst = (ost if q == 0 else abuf, (y_hbm, dx_hbm)[q])
        return pltpu.make_async_copy(src.at[pl.ds(k * R, R)], dst.at[pl.ds(k * R, R)], out_sem.at[q])

    def out_step(q, u, wt, res, out, k):
        acc = conv(u, wt, k * R).reshape(R, TW, C)
        v = acc + res[pl.ds(k * R + 1, R), TB:TB + TW, :].astype(F32)
        out[pl.ds(k * R, R)] = v.astype(BF16)
        out_copy(q, k).start()

    def y_rows(lo, hi, slot, extra=None):
        def step(k):
            sums_at(slot - lo, lo, hi, k)
            with jax.named_scope("y"):
                if extra is not None:
                    extra(k)
                out_step(0, uz, w2, ux, ost, k)
        _loop(lo, hi, step)
    y_rows(0, 1, 9)

    with jax.named_scope("stat1"):
        tot = stat_finish(1)
    vec[2] = tot[0:1]
    vec[3] = tot[1:2]
    outv = [pltpu.make_async_copy(vec.at[2 + q], (dgam_hbm, dbet_hbm)[q], vec_sem.at[q]) for q in range(2)]
    for cp in outv:
        cp.start()
    us = _group_sum(tot * gam) / CNT
    k0 = rstd * gam
    k1 = rstd * rstd * us[0:1]
    k2 = rstd * us[1:2]

    def da_row(r):
        first = last = None
        for i in range(TW // SB):
            sl = pl.ds(i * SB, SB)
            am = abuf[r, sl, :].astype(F32) - mean
            d = dz[r, sl, :] * k0 - (am * k1 + k2)
            ud[r + 1, pl.ds(TB + i * SB, SB), :] = d.astype(BF16)
            first = d[:TB] if first is None else first
            last = d[SB - TB:]
        pad_blocks(3, ud, r, first, last)
        xn[r] = ud[r + 1, TB:TB + TW, :].T

    def da_rows(k):
        for i in range(16):
            da_row((k - 1) * 16 + i)
    y_rows(1, 3, 10, da_rows)
    with jax.named_scope("hstart"):
        halo_start(3, ud)

    def wgrad1_step(t):
        sums_at(12, 0, 9, t)
        with jax.named_scope("tap1"):
            tap(1, ux, xn, t, 0)
    _loop(0, 9, wgrad1_step)
    turn(1, 8)
    with jax.named_scope("hfin_d"):
        halo_row(3, ud)
        halo_cols(3, ud)

    def dx_step(k):
        sums_at(21, 0, 8, k)
        with jax.named_scope("dx"):
            out_step(1, ud, w1t, ug, abuf, k)

    _loop(0, TH // R, dx_step)
    y_rows(3, 8, 29)
    for n, c, k in sorted(plan_at[34], key=lambda e: e[2]):
        ar_step(n, c, k)
    with jax.named_scope("outw"):
        for q in range(2):
            outv[q].wait()
            src, dst = (ost if q == 0 else abuf, (y_hbm, dx_hbm)[q])
            pltpu.make_async_copy(src, dst, out_sem.at[q]).wait()


def finish(y_ref, dx_ref, w1_ref, w2_ref, ga_ref, be_ref, yo, dxo, w1o, w2o, gao, beo,
           yi, dxi, yb, dxb, w1b, w2b, gab, beb, qm, isem, osem):
    nc = 4
    n = TH // nc
    jobs = []
    for k in range(nc):
        part = pl.ds(k * n, n)
        for src, mid, buf, dst in ((dx_ref, dxi, dxb, dxo), (y_ref, yi, yb, yo)):
            jobs.append((src.at[part], mid.at[part], buf.at[part], dst.at[part]))
        if k < 2:
            src, buf, dst = ((w2_ref, w2b, w2o), (w1_ref, w1b, w1o))[k]
            jobs.append((src, buf, None, dst))
    jobs += [(ga_ref, gab, None, gao), (be_ref, beb, None, beo)]
    ins = [pltpu.make_async_copy(src, mid, isem.at[i]) for i, (src, mid, _, _) in enumerate(jobs)]
    for cp in ins:
        cp.start()
    qi = lax.broadcasted_iota(jnp.int32, (TW, TW), 0)
    qj = lax.broadcasted_iota(jnp.int32, (TW, TW), 1)
    qm[:, :] = jnp.where(qi == (qj & 15) * TB + (qj >> 4), 1.0, 0.0).astype(BF16)
    outs = []
    for i, (_, mid, buf, dst) in enumerate(jobs):
        ins[i].wait()
        if buf is not None:
            for r in range(n):
                buf[r] = jnp.dot(qm[:, :], mid[r], preferred_element_type=F32).astype(BF16)
        outs.append(pltpu.make_async_copy(mid if buf is None else buf, dst, osem.at[i]))
        outs[i].start()
    for cp in outs:
        cp.wait()


def solution(mesh):
    tile = P(None, 'h', 'w', None)

    def body(x, w1, gamma, beta, w2, g):
        anyspec = pl.BlockSpec(memory_space=pl.ANY)
        S = jax.ShapeDtypeStruct
        V = pltpu.VMEM
        DMA = pltpu.SemaphoreType.DMA
        img = (TH, TW, C)
        uimg = (TH + 2, EXT, C)
        out = pl.pallas_call(
            kernel,
            out_shape=(S(img, BF16), S(img, BF16), S((3, 3, C, C), F32), S((3, 3, C, C), F32), S((1, C), F32), S((1, C), F32)),
            in_specs=[anyspec] * 6,
            out_specs=(anyspec,) * 6,
            scratch_shapes=[
                V(img, BF16), V(img, BF16), V(uimg, BF16), V(uimg, BF16), V(uimg, BF16), V(uimg, BF16),
                V(img, BF16), V(img, BF16), V(img, F32), V((C, C), F32),
                V((9 * C, C), BF16), V((9 * C, C), BF16), V((9 * C, C), BF16), V((9 * C, C), BF16),
                V((2, 3, 3, C, C), F32), V((2, 3, 3, 128, C), F32), V((2, 3, 2, 3, 32, C), F32), V((2, 3, 2, 3, 16, C), F32),
                V((4, 2, TH, C), F32), V((4, 2, TH, C), F32), V((4, 2, 8, C), F32), V((2, ND, 8, C), F32),
                V((EXT, TW), BF16), V((4, 1, C), F32),
                DMA((2 * NX + 2,)), DMA((2,)), DMA((2,)), DMA((4, 5)), DMA((4, 5)), DMA((2,)), DMA((2,)), DMA((2, 3, 2)), DMA((2, 3, 10)),
            ],
            compiler_params=pltpu.CompilerParams(collective_id=0, has_side_effects=True, vmem_limit_bytes=67043328),
        )(x.reshape(img), w1.reshape(9 * C, C), gamma.reshape(1, C), beta.reshape(1, C), w2.reshape(9 * C, C), g.reshape(img))
        y, dx, dw1, dw2, dgam, dbet = out
        wgt = (9 * C, C)
        row = (1, C)
        shapes = [S(img, BF16), S(img, BF16), S(wgt, F32), S(wgt, F32), S(row, F32), S(row, F32)]
        y, dx, dw1, dw2, dgam, dbet = pl.pallas_call(
            finish,
            out_shape=tuple(shapes),
            in_specs=[anyspec] * 6,
            out_specs=(anyspec,) * 6,
            scratch_shapes=[V(img, BF16), V(img, BF16)] + [V(o.shape, o.dtype) for o in shapes] + [V((TW, TW), BF16), DMA((12,)), DMA((12,))],
            compiler_params=pltpu.CompilerParams(vmem_limit_bytes=67043328),
        )(y, dx, dw1.reshape(wgt), dw2.reshape(wgt), dgam, dbet)
        return (y.reshape(x.shape), dx.reshape(x.shape), dw1.reshape(w1.shape), dw2.reshape(w2.shape), dgam.reshape(C), dbet.reshape(C))

    return jax.shard_map(body, mesh=mesh, in_specs=(tile, P(), P(), P(), P(), tile), out_specs=(tile, tile, P(), P(), P(), P()), check_vma=False)
```

```python
import functools

import jax
import jax.numpy as jnp
from jax import lax
from jax.experimental import pallas as pl
from jax.experimental.pallas import tpu as pltpu
from jax.sharding import PartitionSpec as P

GROUPS = 32
EPS = 1e-5
MESH = pl.DeviceIdType.MESH
F32 = jnp.float32
BF16 = jnp.bfloat16
GC0 = 0.7978845608028654
GC1 = 0.044715
TH, TW, C = 32, 256, 256
CG = C // GROUPS
NW, NH = 4, 2
ND = NW * NH
CNT = float(TH * NH * TW * NW * CG)
TB = 16
EXT = TW + 2 * TB
R = 4
NX = 2


def _group_sum(v):
    lane = lax.broadcasted_iota(jnp.int32, v.shape, 1)
    for k in (1, 2, 4):
        up = pltpu.roll(v, C - k, 1)
        down = pltpu.roll(v, k, 1)
        v = v + jnp.where((lane & k) == 0, up, down)
    return v


def _loop(lo, hi, f):
    def body(i, c):
        f(i)
        return c
    lax.fori_loop(lo, hi, body, 0)


def _row(v):
    return v.sum(0, keepdims=True)


def _fold8(v):
    return v.reshape(v.shape[0] // 8, 8, C).sum(0)


def kernel(x_hbm, w1_hbm, gam_hbm, bet_hbm, w2_hbm, g_hbm,
           y_hbm, dx_hbm, dw1_hbm, dw2_hbm, dgam_hbm, dbet_hbm,
           xn, gn, ux, ug, uz, ud, abuf, ost, dz, raw, w1, w2, w1t, w2t, dw, rd, r1, r2,
           cs, cr, cc, stat, pm, vec,
           in_sem, vec_sem, out_sem, hs_send, hs_recv, st_send, st_recv, ar_send, ar_recv):
    w = lax.axis_index("w")
    h = lax.axis_index("h")
    me = w * NH + h

    rows = TH // NX
    loads = {}
    for q, (src, dst) in enumerate(((x_hbm, xn), (g_hbm, gn))):
        for k in range(NX):
            cp = pltpu.make_async_copy(src.at[pl.ds(k * rows, rows)], dst.at[pl.ds(k * rows, rows)], in_sem.at[q * NX + k])
            cp.start()
            loads[q, k] = cp
        wsrc, wdst = ((w1_hbm, w1), (w2_hbm, w2))[q]
        cp = pltpu.make_async_copy(wsrc, wdst, in_sem.at[2 * NX + q])
        cp.start()
        loads[q, "w"] = cp
        cp = pltpu.make_async_copy((gam_hbm, bet_hbm)[q], vec.at[q], vec_sem.at[q])
        cp.start()
        loads[q, "v"] = cp

    barrier = pltpu.get_barrier_semaphore()
    for k in range(1, ND):
        t = lax.rem(me + k, ND)
        pl.semaphore_signal(barrier, inc=1, device_id={"w": t // NH, "h": lax.rem(t, NH)}, device_id_type=MESH)

    pi = lax.broadcasted_iota(jnp.int32, (EXT, TW), 0)
    pj = lax.broadcasted_iota(jnp.int32, (EXT, TW), 1)
    pm[:, :] = jnp.where(pj == (pi & 15) * TB + (pi >> 4) - 1, 1.0, 0.0).astype(BF16)
    for u in (ux, ug, uz, ud):
        u[pl.ds(33 * h, 1)] = jnp.zeros((1, EXT, C), BF16)

    def no_neighbour(side):
        cr[:, side] = jnp.zeros((4, TH, C), F32)
        cc[:, side] = jnp.zeros((4, 8, C), F32)
    pl.when(w == 0)(lambda: no_neighbour(0))
    pl.when(w == NW - 1)(lambda: no_neighbour(1))

    def to_dev(dw_, dh):
        return {"w": w + dw_, "h": h if dh == 0 else 1 - h}

    def rcopy(src, dst, ss, rs, dev):
        return pltpu.make_async_remote_copy(src_ref=src, dst_ref=dst, send_sem=ss, recv_sem=rs, device_id=dev, device_id_type=MESH)

    def halo_copies(q, u):
        slab = pl.ds(pl.multiple_of(24 * (1 - h), 8), 8)

        def make(m, src, dst, dev):
            return lambda: rcopy(src, dst, hs_send.at[q, m], hs_recv.at[q, m], dev)
        row = make(0, u.at[pl.ds(32 - 31 * h, 1)], u.at[pl.ds(33 * h, 1)], to_dev(0, 1))
        left = [make(1, cs.at[q, 0], cr.at[q, 1], to_dev(-1, 0)), make(2, cs.at[q, 0, slab], cc.at[q, 1], to_dev(-1, 1))]
        right = [make(3, cs.at[q, 1], cr.at[q, 0], to_dev(1, 0)), make(4, cs.at[q, 1, slab], cc.at[q, 0], to_dev(1, 1))]
        return row, left, right

    def halo_start(q, u, row_too=True):
        row, left, right = halo_copies(q, u)
        if row_too:
            row().start()

        @pl.when(w > 0)
        def _():
            for cp in left:
                cp().start()

        @pl.when(w < NW - 1)
        def _():
            for cp in right:
                cp().start()

    sub = lax.broadcasted_iota(jnp.int32, (TB, C), 0)

    def put(u, r, lo, hi):
        b0 = u[r, :TB, :].astype(F32)
        u[r, :TB, :] = jnp.where(sub == 0, lo, b0).astype(BF16)
        b1 = u[r, TW + TB:, :].astype(F32)
        u[r, TW + TB:, :] = jnp.where(sub == TB - 1, hi, b1).astype(BF16)

    def halo_row(q, u):
        halo_copies(q, u)[0]().wait()

    def halo_cols(q, u):
        _, left, right = halo_copies(q, u)

        @pl.when(w > 0)
        def _():
            for cp in left:
                cp().wait_send()
            for cp in right:
                cp().wait_recv()

        @pl.when(w < NW - 1)
        def _():
            for cp in right:
                cp().wait_send()
            for cp in left:
                cp().wait_recv()

        def step(k):
            for i in range(8):
                r = k * 8 + i
                put(u, r + 1, cr[q, 0, pl.ds(r, 1), :], cr[q, 1, pl.ds(r, 1), :])
        _loop(0, TH // 8, step)
        put(u, 33 * (1 - h), cc[q, 0, pl.ds(7 * h, 1), :], cc[q, 1, pl.ds(7 * h, 1), :])

    def permute_in(q, src, u):
        for k in range(NX):
            if q == 1:
                loads[q, k].wait()

            def step(i):
                for d in range(16):
                    r = k * rows + i * 16 + d
                    v = jnp.dot(pm[:, :], src[r], preferred_element_type=F32)
                    u[r + 1] = v.astype(BF16)
                    if q == 1:
                        cs[q, 0, pl.ds(r, 1), :] = v[TB:TB + 1]
                        cs[q, 1, pl.ds(r, 1), :] = v[TW + TB - 1:TW + TB]
            _loop(0, rows // 16, step)

    def pad_blocks(q, u, r, first, last):
        u[r + 1, :TB, :] = jnp.where(sub == 0, 0.0, pltpu.roll(last, 1, 0)).astype(BF16)
        u[r + 1, TW + TB:, :] = jnp.where(sub == TB - 1, 0.0, pltpu.roll(first, TB - 1, 0)).astype(BF16)
        cs[q, 0, pl.ds(r, 1), :] = first[0:1]
        cs[q, 1, pl.ds(r, 1), :] = last[TB - 1:TB]

    def conv(u, wt, r0, R=R):
        lhs = jnp.concatenate([u[pl.ds(r0 + a, R), TB * b:TB * b + TW, :].reshape(R * TW, C) for a in range(3) for b in range(3)], axis=1)
        return jnp.dot(lhs, wt[:, :], preferred_element_type=F32)

    def stat_copies(q):
        out = []
        for k in range(1, ND):
            t = lax.rem(me + k, ND)
            out.append(rcopy(stat.at[q, me], stat.at[q, me], st_send.at[q], st_recv.at[q], {"w": t // NH, "h": lax.rem(t, NH)}))
        return out

    def stat_start(q, a, b):
        stat[q, me] = jnp.concatenate([a, b, jnp.zeros((6, C), F32)], axis=0)
        for cp in stat_copies(q):
            cp.start()

    def stat_finish(q):
        others = stat.at[q, pl.ds(0, ND - 1)]
        rcopy(others, others, st_send.at[q], st_recv.at[q], dev_c).wait()
        tot = stat[q, 0]
        for k in range(1, ND):
            tot = tot + stat[q, k]
        return tot

    xb = lax.rem(w, 2)
    yb = w // 2
    dev_x = {"w": w + 1 - 2 * xb, "h": h}
    dev_y = {"w": w + 2 - 4 * yb, "h": h}
    dev_c = {"w": w, "h": 1 - h}

    BS = (1, 0, 2)

    def part(n, c, off, size):
        return dw.at[n, c, :, pl.ds(pl.multiple_of(off, 16), size), :]

    def half(n, c, off, size):
        return rd.at[n, c, :, pl.ds(pl.multiple_of(off, 16), size), :]

    def ar_copies(n, c):
        mine, other = 128 * h, 128 * (1 - h)
        o0, o1 = 32 * xb + 16 * yb, 64 + 32 * yb + 16 * xb
        q0, q1 = 32 * xb, 64 + 32 * yb
        out = (dw2_hbm, dw1_hbm)[n].at[:, BS[c], pl.ds(pl.multiple_of(mine, 128), 128), :]
        plan = (
            (part(n, c, other, 128), rd.at[n, c], dev_c),
            (part(n, c, mine + 32 * (1 - xb), 32), r1.at[n, c, 0], dev_x),
            (part(n, c, mine + 64 + 32 * (1 - yb), 32), r1.at[n, c, 1], dev_y),
            (part(n, c, mine + 32 * xb + 16 * (1 - yb), 16), r2.at[n, c, 0], dev_y),
            (part(n, c, mine + 64 + 32 * yb + 16 * (1 - xb), 16), r2.at[n, c, 1], dev_x),
            (half(n, c, o0, 16), half(n, c, o0, 16), dev_y),
            (half(n, c, o1, 16), half(n, c, o1, 16), dev_x),
            (half(n, c, q0, 32), half(n, c, q0, 32), dev_x),
            (half(n, c, q1, 32), half(n, c, q1, 32), dev_y),
            (rd.at[n, c], out, dev_c),
        )

        def make(k):
            src, dst, dev = plan[k]
            return lambda: rcopy(src, dst, ar_send.at[n, c, k % 2], ar_recv.at[n, c, k], dev)
        return [make(k) for k in range(10)] + [lambda: pltpu.make_async_copy(rd.at[n, c], out, in_sem.at[n * 3 + c])]

    AR_SETS = ((0,), (1, 2), (3, 4), (5, 6), (7, 8), (9, 10))

    def accumulate(n, c, off, size, src, into=None):
        sl = pl.ds(pl.multiple_of(128 * h + off, 16), size)
        for t in range(3):
            v = dw[n, c, t, sl, :] + src[t]
            if into is None:
                dw[n, c, t, sl, :] = v
            else:
                rd[n, c, t, pl.ds(pl.multiple_of(off, 16), size), :] = v

    def ar_step(n, c, k):
        with jax.named_scope(f"ar_{n}_{c}_{k}"):
            cps = ar_copies(n, c)
            if k > 0:
                for i in AR_SETS[k - 1]:
                    cps[i]().wait()
            if k == 1:
                accumulate(n, c, 0, 128, rd.at[n, c])
            if k == 2:
                accumulate(n, c, 32 * xb, 32, r1.at[n, c, 0])
                accumulate(n, c, 64 + 32 * yb, 32, r1.at[n, c, 1])
            if k == 3:
                accumulate(n, c, 32 * xb + 16 * yb, 16, r2.at[n, c, 0], rd)
                accumulate(n, c, 64 + 32 * yb + 16 * xb, 16, r2.at[n, c, 1], rd)
            if k < 6:
                for i in AR_SETS[k]:
                    cps[i]().start()

    SLOTS = "347:?FI79<@CKQ:;>AHNQ@BGJMQRCEILNRREFILORR"
    plan_at = {}
    for i_, ch_ in enumerate(SLOTS):
        plan_at.setdefault(ord(ch_) - ord("0"), []).append((i_ // 21, i_ // 7 % 3, i_ % 7))

    def sums_at(base, lo, hi, i):
        for sl in range(lo, hi):
            if sl + base in plan_at:
                def _(todo=plan_at[sl + base]):
                    for n, c, k in sorted(todo, key=lambda e: -e[2]):
                        ar_step(n, c, k)
                pl.when(i == sl)(_)

    def perm3(i):
        return (3 * i * i - 5 * i + 2) // 2

    def turn(n, t):
        dw[n, t // 3, perm3(t % 3)] = raw[:, :].T

    def tap(n, u, vt, t, first):
        turn(n, lax.max(t - 1, first))
        rhs = u[pl.ds(perm3(t % 3), TH), pl.ds(pl.multiple_of(TB * perm3(t // 3), TB), TW), :].reshape(TH * TW, C)
        lhs = jnp.concatenate([vt[r] for r in range(TH)], axis=1)
        raw[:, :] = jnp.dot(lhs, rhs, preferred_element_type=F32)

    def x_edges(i):
        for d in range(16):
            r = i * 16 + d
            cs[0, 0, pl.ds(r, 1), :] = xn[r, :TB, :].astype(F32)[:1]
            cs[0, 1, pl.ds(r, 1), :] = xn[r, TW - TB:, :].astype(F32)[TB - 1:]
    with jax.named_scope("edges"):
        for k in range(NX):
            loads[0, k].wait()
        _loop(0, TH // 16, x_edges)
    with jax.named_scope("barrier"):
        pl.semaphore_wait(barrier, ND - 1)
    halo_start(0, ux, False)
    with jax.named_scope("perm_x"):
        permute_in(0, xn, ux)
    halo_copies(0, ux)[0]().start()
    with jax.named_scope("perm_g"):
        permute_in(1, gn, ug)
    halo_start(1, ug)
    loads[0, "w"].wait()
    loads[1, "w"].wait()
    with jax.named_scope("hfin_x"):
        halo_row(0, ux)
        halo_cols(0, ux)

    def wtrans(k):
        for i in range(3):
            t = lax.min(k * 3 + i, 8)
            src, dst = pl.ds(pl.multiple_of(t * C, C), C), pl.ds(pl.multiple_of((8 - t) * C, C), C)
            w1t[dst, :] = w1[src, :].T
            w2t[dst, :] = w2[src, :].T

    def conv1_step(k, carry):
        s1, s2 = carry
        wtrans(k)
        a = conv(ux, w1, k * 8, 8).astype(BF16)
        abuf[pl.ds(k * 8, 8)] = a.reshape(8, TW, C)
        af = a.astype(F32)
        return s1 + _fold8(af), s2 + _fold8(af * af)
    zero = jnp.zeros((8, C), F32)
    with jax.named_scope("conv1"):
        s1, s2 = lax.fori_loop(0, TH // 8, conv1_step, (zero, zero))
    with jax.named_scope("ststart"):
        stat_start(0, _row(s1), _row(s2))
    with jax.named_scope("hfin_g"):
        halo_row(1, ug)
        halo_cols(1, ug)

    def convt2(k, R=R):
        dz[pl.ds(k * R, R)] = conv(ug, w2t, k * R, R).reshape(R, TW, C)
        for i in range(R):
            r = k * R + i
            gn[r] = ug[r + 1, TB:TB + TW, :].T
    with jax.named_scope("convt2"):
        _loop(0, 2, lambda k: convt2(k, 2 * R))

    with jax.named_scope("stat0"):
        tot = _group_sum(stat_finish(0)) / CNT
    mean = tot[0:1]
    rstd = lax.rsqrt(tot[1:2] - mean * mean + EPS)
    loads[0, "v"].wait()
    loads[1, "v"].wait()
    gam = vec[0]
    bet = vec[1]
    ngain = rstd * gam

    SB = TB

    def gate(r, sl):
        am = abuf[r, sl, :].astype(F32) - mean
        n = am * ngain + bet
        n2 = n * n
        th = jnp.tanh(n * (n2 * (GC0 * GC1) + GC0))
        return am, n, n2, 0.5 * th + 0.5

    def slope(n, n2, hp):
        return hp + n * ((hp - hp * hp) * (n2 * (6.0 * GC0 * GC1) + 2.0 * GC0))

    def act_row(r, carry, do_z, do_dn):
        t0, t1 = carry
        first = last = None
        for i in range(TW // SB):
            sl = pl.ds(i * SB, SB)
            am, n, n2, hp = gate(r, sl)
            if do_z:
                z = n * hp
                uz[r + 1, pl.ds(TB + i * SB, SB), :] = z.astype(BF16)
                first = z[:TB] if first is None else first
                last = z[SB - TB:]
            if do_dn:
                dn = dz[r, sl, :] * slope(n, n2, hp)
                dz[r, sl, :] = dn
                t0 = t0 + _fold8(dn * am)
                t1 = t1 + _fold8(dn)
        if do_z:
            pad_blocks(2, uz, r, first, last)
        return t0, t1

    def convt2_z(k):
        with jax.named_scope("convt2z"):
            for i in range(8):
                act_row((k - 4) * 8 + i, (zero, zero), True, False)
            convt2(k)
    _loop(4, 8, convt2_z)
    with jax.named_scope("hstart"):
        halo_start(2, uz)
    raw[:, :] = jnp.zeros((C, C), F32)

    def tap2(lo, hi, first, rows, carry):
        def step(t, c):
            sums_at(0, lo, hi, t)
            if lo == 0:
                @pl.when(t == 1)
                def _():
                    with jax.named_scope("hrow_z"):
                        halo_row(2, uz)
            with jax.named_scope("tap2"):
                for i in range(rows):
                    c = act_row((t - lo) * rows + i, c, False, True)
                tap(0, uz, gn, t, first)
            return c
        return lax.fori_loop(lo, hi, step, carry)

    sums = tap2(0, 3, 0, 0, (zero, zero))
    turn(0, 2)
    with jax.named_scope("hcol_z"):
        halo_cols(2, uz)
    sums = tap2(3, 7, 3, 8, sums)
    with jax.named_scope("ststart"):
        stat_start(1, _row(sums[0]) * rstd, _row(sums[1]))
    tap2(7, 9, 3, 0, zero)
    turn(0, 8)

    def out_copy(q, k):
        src, dst = (ost if q == 0 else abuf, (y_hbm, dx_hbm)[q])
        return pltpu.make_async_copy(src.at[pl.ds(k * R, R)], dst.at[pl.ds(k * R, R)], out_sem.at[q])

    def out_step(q, u, wt, res, out, k):
        acc = conv(u, wt, k * R).reshape(R, TW, C)
        v = acc + res[pl.ds(k * R + 1, R), TB:TB + TW, :].astype(F32)
        out[pl.ds(k * R, R)] = v.astype(BF16)
        out_copy(q, k).start()

    def y_rows(lo, hi, slot, extra=None):
        def step(k):
            sums_at(slot - lo, lo, hi, k)
            with jax.named_scope("y"):
                if extra is not None:
                    extra(k)
                out_step(0, uz, w2, ux, ost, k)
        _loop(lo, hi, step)
    y_rows(0, 1, 9)

    with jax.named_scope("stat1"):
        tot = stat_finish(1)
    vec[2] = tot[0:1]
    vec[3] = tot[1:2]
    outv = [pltpu.make_async_copy(vec.at[2 + q], (dgam_hbm, dbet_hbm)[q], vec_sem.at[q]) for q in range(2)]
    for cp in outv:
        cp.start()
    us = _group_sum(tot * gam) / CNT
    k0 = rstd * gam
    k1 = rstd * rstd * us[0:1]
    k2 = rstd * us[1:2]

    def da_row(r):
        first = last = None
        for i in range(TW // SB):
            sl = pl.ds(i * SB, SB)
            am = abuf[r, sl, :].astype(F32) - mean
            d = dz[r, sl, :] * k0 - (am * k1 + k2)
            ud[r + 1, pl.ds(TB + i * SB, SB), :] = d.astype(BF16)
            first = d[:TB] if first is None else first
            last = d[SB - TB:]
        pad_blocks(3, ud, r, first, last)
        xn[r] = ud[r + 1, TB:TB + TW, :].T

    def da_rows(k):
        for i in range(16):
            da_row((k - 1) * 16 + i)
    y_rows(1, 3, 10, da_rows)
    with jax.named_scope("hstart"):
        halo_start(3, ud)

    def wgrad1_step(t):
        sums_at(12, 0, 9, t)
        with jax.named_scope("tap1"):
            tap(1, ux, xn, t, 0)
    _loop(0, 9, wgrad1_step)
    turn(1, 8)
    with jax.named_scope("hfin_d"):
        halo_row(3, ud)
        halo_cols(3, ud)

    def dx_step(k):
        sums_at(21, 0, 8, k)
        with jax.named_scope("dx"):
            out_step(1, ud, w1t, ug, abuf, k)

    _loop(0, TH // R, dx_step)
    y_rows(3, 8, 29)
    for n, c, k in sorted(plan_at[34], key=lambda e: e[2]):
        ar_step(n, c, k)
    with jax.named_scope("outw"):
        for q in range(2):
            outv[q].wait()
            src, dst = (ost if q == 0 else abuf, (y_hbm, dx_hbm)[q])
            pltpu.make_async_copy(src, dst, out_sem.at[q]).wait()


def finish(y_ref, dx_ref, w1_ref, w2_ref, ga_ref, be_ref, yo, dxo, w1o, w2o, gao, beo,
           yi, dxi, yb, dxb, w1b, w2b, gab, beb, qm, isem, osem):
    nc = 8
    n = TH // nc
    jobs = []
    for k in range(nc):
        part = pl.ds(k * n, n)
        for src, mid, buf, dst in ((dx_ref, dxi, dxb, dxo), (y_ref, yi, yb, yo)):
            jobs.append((src.at[part], mid.at[part], buf.at[part], dst.at[part]))
        if k < 2:
            src, buf, dst = ((w2_ref, w2b, w2o), (w1_ref, w1b, w1o))[k]
            jobs.append((src, buf, None, dst))
    jobs += [(ga_ref, gab, None, gao), (be_ref, beb, None, beo)]
    ins = [pltpu.make_async_copy(src, mid, isem.at[i]) for i, (src, mid, _, _) in enumerate(jobs)]
    for cp in ins:
        cp.start()
    qi = lax.broadcasted_iota(jnp.int32, (TW, TW), 0)
    qj = lax.broadcasted_iota(jnp.int32, (TW, TW), 1)
    qm[:, :] = jnp.where(qi == (qj & 15) * TB + (qj >> 4), 1.0, 0.0).astype(BF16)
    outs = []
    for i, (_, mid, buf, dst) in enumerate(jobs):
        ins[i].wait()
        if buf is not None:
            for r in range(n):
                buf[r] = jnp.dot(qm[:, :], mid[r], preferred_element_type=F32).astype(BF16)
        outs.append(pltpu.make_async_copy(mid if buf is None else buf, dst, osem.at[i]))
        outs[i].start()
    for cp in outs:
        cp.wait()


def solution(mesh):
    tile = P(None, 'h', 'w', None)

    def body(x, w1, gamma, beta, w2, g):
        anyspec = pl.BlockSpec(memory_space=pl.ANY)
        S = jax.ShapeDtypeStruct
        V = pltpu.VMEM
        DMA = pltpu.SemaphoreType.DMA
        img = (TH, TW, C)
        uimg = (TH + 2, EXT, C)
        out = pl.pallas_call(
            kernel,
            out_shape=(S(img, BF16), S(img, BF16), S((3, 3, C, C), F32), S((3, 3, C, C), F32), S((1, C), F32), S((1, C), F32)),
            in_specs=[anyspec] * 6,
            out_specs=(anyspec,) * 6,
            scratch_shapes=[
                V(img, BF16), V(img, BF16), V(uimg, BF16), V(uimg, BF16), V(uimg, BF16), V(uimg, BF16),
                V(img, BF16), V(img, BF16), V(img, F32), V((C, C), F32),
                V((9 * C, C), BF16), V((9 * C, C), BF16), V((9 * C, C), BF16), V((9 * C, C), BF16),
                V((2, 3, 3, C, C), F32), V((2, 3, 3, 128, C), F32), V((2, 3, 2, 3, 32, C), F32), V((2, 3, 2, 3, 16, C), F32),
                V((4, 2, TH, C), F32), V((4, 2, TH, C), F32), V((4, 2, 8, C), F32), V((2, ND, 8, C), F32),
                V((EXT, TW), BF16), V((4, 1, C), F32),
                DMA((2 * NX + 2,)), DMA((2,)), DMA((2,)), DMA((4, 5)), DMA((4, 5)), DMA((2,)), DMA((2,)), DMA((2, 3, 2)), DMA((2, 3, 10)),
            ],
            compiler_params=pltpu.CompilerParams(collective_id=0, has_side_effects=True, vmem_limit_bytes=67043328),
        )(x.reshape(img), w1.reshape(9 * C, C), gamma.reshape(1, C), beta.reshape(1, C), w2.reshape(9 * C, C), g.reshape(img))
        y, dx, dw1, dw2, dgam, dbet = out
        wgt = (9 * C, C)
        row = (1, C)
        shapes = [S(img, BF16), S(img, BF16), S(wgt, F32), S(wgt, F32), S(row, F32), S(row, F32)]
        y, dx, dw1, dw2, dgam, dbet = pl.pallas_call(
            finish,
            out_shape=tuple(shapes),
            in_specs=[anyspec] * 6,
            out_specs=(anyspec,) * 6,
            scratch_shapes=[V(img, BF16), V(img, BF16)] + [V(o.shape, o.dtype) for o in shapes] + [V((TW, TW), BF16), DMA((20,)), DMA((20,))],
            compiler_params=pltpu.CompilerParams(vmem_limit_bytes=67043328),
        )(y, dx, dw1.reshape(wgt), dw2.reshape(wgt), dgam, dbet)
        return (y.reshape(x.shape), dx.reshape(x.shape), dw1.reshape(w1.shape), dw2.reshape(w2.shape), dgam.reshape(C), dbet.reshape(C))

    return jax.shard_map(body, mesh=mesh, in_specs=(tile, P(), P(), P(), P(), tile), out_specs=(tile, tile, P(), P(), P(), P()), check_vma=False)
```
